256 devices in a mesh: tm: 64 (over z, x, core), asset: 4 (over y).
Axes of the slice: x: 4, y: 4, z: 8, core: 2. Of those that a mesh axis runs over, the one named last changes fastest.
Arguments:
- returns: float32 [1024, 2048], P('tm', 'asset'), may hold values from -6 to 6
- windows: int32 [64], P('tm'), may hold values from 20 to 250, as said below
- listed_from: int32 [2048], replicated, may hold values from 0 to 511
- listed_until: int32 [2048], replicated, may hold values from 512 to 1024
Outputs:
- correlation: float32 [64, 2048, 2048], P('tm', None, 'asset')
The draws below stay inside these ranges and needn't reach their ends.
Inputs may be any that keep to these rules, and one draw needn't show every extreme that they name: `windows`: each window length is one of the four horizons max(256 * h // 256, 2) for h in 20, 60, 120, 250; the shortest and the longest both occur in every draw.
All inputs are finite; a program needn't handle non-finite values.
Results may differ from the reference program's by a relative error of at most 0.0003.
Values sent between devices are 32-bit elements; how exact they have to be, the bound alone decides.
A program may use at most 128 MiB of HBM per device.

```python
import jax
import jax.numpy as jnp
from jax import lax

ASSETS = 2048
SPAN = 256
GROUP = 16
DAYS = 1024
N_TM = 64


def draw_windows(key, part):
    horizons = jnp.array([20, 60, 120, 250], jnp.int32)
    key_pick = jax.random.fold_in(key, 11)
    key_spot = jax.random.fold_in(key, 23)
    chosen_idx = jax.random.randint(key_pick, (N_TM,), 0, 4)
    special = jax.random.randint(key_spot, (), 0, N_TM)
    position = jnp.arange(N_TM, dtype=jnp.int32)
    chosen_idx = jnp.where(position == special, 3, chosen_idx)
    chosen_idx = jnp.where(position == (special + 1) % N_TM, 0, chosen_idx)
    lengths = jnp.sum(jnp.where(chosen_idx[:, None] == jnp.arange(4, dtype=jnp.int32)[None, :], horizons[None, :], 0), axis=1)
    return jnp.maximum(SPAN * lengths // 256, 2).astype(jnp.int32)


def set_ends(values, own_key, low, high):
    index_at = [jax.random.randint(jax.random.fold_in(own_key, axis), (), 0, length) for axis, length in enumerate(values.shape)]
    main_axis = values.shape.index(max(values.shape))
    neighbour = index_at[:main_axis] + [(index_at[main_axis] + 1) % values.shape[main_axis]] + index_at[main_axis + 1:]
    return values.at[tuple(index_at)].set(low).at[tuple(neighbour)].set(high)


def shard_levels(own_key, extent, cuts, low, largest):
    factor_of, own = 1.0, jax.random.fold_in(own_key, 6)
    for dim, shards_of in cuts:
        steps = jnp.exp(jax.random.uniform(jax.random.fold_in(own, dim), (shards_of,), jnp.float32, low / len(cuts), largest / len(cuts)))
        factor_of = factor_of * jnp.repeat(steps, extent[dim] // shards_of).reshape([-1 if axis == dim else 1 for axis in range(len(extent))])
    return factor_of


def gaussian(own_key, shape, deviation, most, shards=(), kind=jnp.bfloat16):
    values = deviation * jax.random.normal(own_key, shape, jnp.float32)
    if shards:
        values = values * shard_levels(own_key, shape, shards, -0.22, 0.18)
    return jnp.clip(values, -most, most).astype(kind)


def setup_inputs(seed: int = 0) -> dict:
    key_of = jax.random.split(jax.random.key(seed), 5)
    return {
        "returns": gaussian(key_of[0], (DAYS, ASSETS), 1.0, 6.0, ((0, 64), (1, 4)), jnp.float32),
        "windows": draw_windows(jax.random.fold_in(key_of[4], 71), 0),
        "listed_from": set_ends(jax.random.randint(key_of[2], (ASSETS,), 0, DAYS // 2), jax.random.fold_in(key_of[2], 1), 0, (DAYS // 2) - 1).astype(jnp.int32),
        "listed_until": set_ends(jax.random.randint(key_of[3], (ASSETS,), DAYS // 2, DAYS + 1), jax.random.fold_in(key_of[3], 1), DAYS // 2, DAYS).astype(jnp.int32),
    }


highest = lax.Precision.HIGHEST

def cross_days(left_side, right_side):
    return lax.dot_general(left_side, right_side, (((0,), (0,)), ((), ())), precision=highest, preferred_element_type=jnp.float32)

def correlate(cross_terms, sum_left, sum_right, square_left, square_right, pair_count):
    pairs = jnp.maximum(pair_count, 1.0)
    covariance = cross_terms - sum_left * sum_right / pairs
    var_left = jnp.maximum(square_left - sum_left * sum_left / pairs, 1.0)
    var_right = jnp.maximum(square_right - sum_right * sum_right / pairs, 1.0)
    return covariance / jnp.sqrt(var_left * var_right)

def reference(returns, windows, listed_from, listed_until):
    padded = jnp.concatenate([jnp.zeros((SPAN - GROUP, ASSETS), jnp.float32), returns], axis=0)

    def evaluate(evaluation):
        end_day = (evaluation + 1) * GROUP - 1
        window_rows = lax.dynamic_slice_in_dim(padded, (evaluation * GROUP).astype(jnp.int32), SPAN, 0)
        day_index = end_day - SPAN + 1 + jnp.arange(SPAN, dtype=jnp.int32)
        inside = (day_index > end_day - windows[evaluation]) & (day_index >= 0)
        alive = inside[:, None] & (listed_from[None, :] <= day_index[:, None]) & (day_index[:, None] < listed_until[None, :])
        listed = alive.astype(jnp.float32)
        values = window_rows * listed
        squared = values * values
        cross_terms = cross_days(values, values)
        sum_terms = cross_days(values, listed)
        square_terms = cross_days(squared, listed)
        pair_count = cross_days(listed, listed)
        return correlate(cross_terms, sum_terms, sum_terms.T, square_terms, square_terms.T, pair_count)
    return lax.map(evaluate, jnp.arange(N_TM, dtype=jnp.int32))
```

```python
import functools

import jax
import jax.numpy as jnp
from jax import lax
from jax.experimental import pallas as pl
from jax.experimental.pallas import tpu as pltpu
from jax.sharding import PartitionSpec as P

MESH = pl.DeviceIdType.MESH
F32, BF16 = jnp.float32, jnp.bfloat16
NZ, NX, NY = 8, 4, 4
GROUP, HALF, SPAN = 16, 8, 256
COLS, ASSETS = 512, 2048

Z_SEM = 0
YS_SEM = Z_SEM + 4
YSR_SEM = YS_SEM + 12
XA_SEM = YSR_SEM + 6
XAR_SEM = XA_SEM + 4
XB_SEM = XAR_SEM + 2
XBR_SEM = XB_SEM + 16
YA_SEM = XBR_SEM + 8
YAR_SEM = YA_SEM + 6
D_SEM = YAR_SEM + 6
N_SEM = D_SEM + 8


def gather_kernel(returns_ref, all_ref, own, ss, rs, local_sem):
    tm, y = lax.axis_index("tm"), lax.axis_index("asset")
    z, x, c = tm // 8, (tm // 2) % 4, tm % 2

    def dev(dz=0, dx=0, dy=0, dc=0):
        return (
            ((z + dz) % NZ) * 8 + ((x + dx) % NX) * 2 + (c + dc) % 2,
            (y + dy) % NY,
        )

    partner = dev(dc=1)

    def copy(src, dst, i, to):
        return pltpu.make_async_remote_copy(
            src_ref=src, dst_ref=dst, send_sem=ss.at[i], recv_sem=rs.at[i], device_id=to, device_id_type=MESH
        )

    def received(dst, i):
        copy(dst, dst, i, partner).wait_recv()

    def send(src, dst, i, to):
        copy(src, dst, i, to).start()

    loads = [
        pltpu.make_async_copy(returns_ref.at[pl.ds(h * HALF, HALF)], own.at[h, y, 0], local_sem.at[h]) for h in (0, 1)
    ]
    for load in loads:
        load.start()
    barrier = pltpu.get_barrier_semaphore()
    peers = [dev(dz=1), dev(dz=-1), dev(dz=2), dev(dz=-2), dev(dx=1), dev(dx=-1), dev(dy=1), dev(dy=-1), partner]
    for peer in peers:
        pl.semaphore_signal(barrier, inc=1, device_id=peer, device_id_type=MESH)
    pl.semaphore_wait(barrier, len(peers))
    for load in loads:
        load.wait()

    step = (1, -1)

    def ring_x(dx):
        return (x + dx) % NX

    def z_send(h, k):
        send(own.at[h, y, 0], own.at[h, y, k], Z_SEM + h * 2 + k - 1, dev(dz=k))

    def z_wait(k):
        for h in (0, 1):
            received(own.at[h, y, k], Z_SEM + h * 2 + k - 1)

    def ys_send(k):
        for h in (0, 1):
            for d in (0, 1):
                send(own.at[h, y, k], own.at[h, y, k], YS_SEM + h * 6 + k * 2 + d, dev(dy=step[d]))

    def ys_wait(k):
        for h in (0, 1):
            for d in (0, 1):
                origin = (y - step[d]) % NY
                received(own.at[h, origin, k], YS_SEM + h * 6 + k * 2 + d)
                if (h + k) % 2 == d:
                    send(own.at[h, origin, k], own.at[h, origin, k], YSR_SEM + h * 3 + k, dev(dy=step[d]))

    def ysr_wait(k):
        for h in (0, 1):
            received(own.at[h, (y + 2) % NY, k], YSR_SEM + h * 3 + k)

    def x_send(h, j, k):
        base = XA_SEM if h == 0 else XB_SEM + j * 4
        at = (y + j) % NY
        for d in (0, 1):
            to = ring_x(step[d])
            up = to > x

            def go(slot):
                send(
                    own.at[h, at, k],
                    all_ref.at[at, c, h, x, slot],
                    base + d * 2 + slot,
                    dev(dx=step[d]),
                )

            if k == 1:
                go(up.astype(jnp.int32))
            elif k == 0:
                pl.when(up)(lambda: go(0))
            else:
                pl.when(jnp.logical_not(up))(lambda: go(1))

    def x_wait(h, j):
        base, relay = (XA_SEM, XAR_SEM) if h == 0 else (XB_SEM + j * 4, XBR_SEM + j * 2)
        at = (y + j) % NY
        first = (jnp.where(x == 3, 1, 0), jnp.where(x == 0, 0, 1))
        for d in (0, 1):
            origin = ring_x(-step[d])
            received(all_ref.at[at, c, h, origin, first[d]], base + d * 2 + first[d])
            send(all_ref.at[at, c, h, origin, first[d]], all_ref.at[at, c, h, origin, d], relay + d, dev(dx=step[d]))
        for d in (0, 1):
            origin = ring_x(-step[d])
            received(all_ref.at[at, c, h, origin, 1 - first[d]], base + d * 2 + 1 - first[d])

    def xr_wait(h, j):
        relay = XAR_SEM if h == 0 else XBR_SEM + j * 2
        at = (y + j) % NY
        for d in (0, 1):
            received(all_ref.at[at, c, h, ring_x(2), d], relay + d)

    def ya_send(dist):
        at = ring_x(-dist)
        for d in (0, 1):
            view = all_ref.at[y, c, 0, at]
            send(view, view, YA_SEM + (dist - 1) * 2 + d, dev(dy=step[d]))

    def ya_wait(dist):
        at = ring_x(-dist)
        for d in (0, 1):
            origin = (y - step[d]) % NY
            received(all_ref.at[origin, c, 0, at], YA_SEM + (dist - 1) * 2 + d)
            view = all_ref.at[origin, c, 0, at, d]
            send(view, view, YAR_SEM + (dist - 1) * 2 + d, dev(dy=step[d]))

    def yar_wait(dist):
        at = ring_x(-dist)
        for d in (0, 1):
            received(all_ref.at[(y + 2) % NY, c, 0, at, d], YAR_SEM + (dist - 1) * 2 + d)

    def to_partner(h, dist):
        at = ring_x(-dist)
        if dist == 0:
            send(own.at[h, :, pl.ds(c, 2)], all_ref.at[:, c, h, x], D_SEM + h * 4, partner)
        else:
            send(all_ref.at[:, c, h, at], all_ref.at[:, c, h, at], D_SEM + h * 4 + dist, partner)

    def from_partner(h, dist):
        received(all_ref.at[:, 1 - c, h, ring_x(-dist)], D_SEM + h * 4 + dist)

    for k in (1, 2):
        for h in (0, 1):
            z_send(h, k)
    ys_send(0)
    x_send(0, 0, 0)
    x_send(1, 0, 0)
    ys_wait(0)
    x_send(1, 1, 0)
    x_send(1, 3, 0)
    z_wait(1)
    x_send(0, 0, 1)
    ys_send(1)
    x_send(1, 0, 1)
    z_wait(2)
    x_send(0, 0, 2)
    ys_send(2)
    x_send(1, 0, 2)
    ysr_wait(0)
    x_send(1, 2, 0)
    ys_wait(1)
    x_send(1, 1, 1)
    x_send(1, 3, 1)
    x_wait(0, 0)
    ya_send(1)
    ya_send(3)
    ys_wait(2)
    x_send(1, 1, 2)
    x_send(1, 3, 2)
    x_wait(1, 0)
    ysr_wait(1)
    x_send(1, 2, 1)
    xr_wait(0, 0)
    ya_send(2)
    ysr_wait(2)
    x_send(1, 2, 2)
    to_partner(0, 0)
    to_partner(1, 0)
    all_ref[:, pl.ds(c, 1), :, pl.ds(x, 1)] = jnp.swapaxes(own[:, :, 0:2], 0, 1)[:, None, :, None]
    x_wait(1, 1)
    x_wait(1, 3)
    ya_wait(1)
    ya_wait(3)
    x_wait(1, 2)
    to_partner(1, 1)
    to_partner(1, 3)
    ya_wait(2)
    for j in range(4):
        xr_wait(1, j)
    to_partner(1, 2)
    yar_wait(1)
    to_partner(0, 1)
    yar_wait(3)
    to_partner(0, 3)
    yar_wait(2)
    to_partner(0, 2)
    for h, dist in ((0, 0), (1, 0), (1, 1), (1, 3), (1, 2), (0, 1), (0, 3), (0, 2)):
        from_partner(h, dist)

    block, two = own.at[0, 0, 0], own.at[0, 0, pl.ds(0, 2)]
    many = all_ref.at[:, 0, 0, 0]
    for i in range(N_SEM):
        view = many if i >= D_SEM else two if YA_SEM <= i < YAR_SEM else block
        copy(view, view, i, partner).wait_send()


def gathered(returns):
    return pl.pallas_call(
        gather_kernel,
        out_shape=jax.ShapeDtypeStruct((NY, 2, 2, NX, 2, HALF, COLS), F32),
        in_specs=[pl.BlockSpec(memory_space=pl.ANY)],
        out_specs=pl.BlockSpec(memory_space=pltpu.VMEM),
        scratch_shapes=[
            pltpu.VMEM((2, NY, 3, HALF, COLS), F32),
            pltpu.SemaphoreType.DMA((N_SEM,)),
            pltpu.SemaphoreType.DMA((N_SEM,)),
            pltpu.SemaphoreType.DMA((2,)),
        ],
        compiler_params=pltpu.CompilerParams(collective_id=0, has_side_effects=True),
    )(returns)


def day_of(row, tm):
    core, half, at, slot, day = row // 128, (row // 64) % 2, (row // 16) % 4, (row // 8) % 2, row % 8
    place = at * 2 + core
    back = slot + (place > tm % 8).astype(jnp.int32)
    return ((tm // 8 - back) * 8 + place) * GROUP + half * HALF + day


def split(value):
    high = value.astype(BF16)
    return high, (value - high.astype(F32)).astype(BF16)


def dot(left, right):
    return jnp.dot(left, right, preferred_element_type=F32)


ROWS = 256
TILE = 256


def correlate_kernel(windows_ref, from_ref, until_ref, all_ref, out_ref, high_r, low_r, live_r, sq_high_r, sq_low_r):
    tm, y = lax.axis_index("tm"), lax.axis_index("asset")
    g = pl.program_id(0)
    end = (tm + 1) * GROUP
    begin = jnp.maximum(end - windows_ref[0], 0)

    def spans(at, width):
        first = jnp.maximum(from_ref[:, pl.ds(at, width)], begin).astype(F32)
        last = jnp.minimum(until_ref[:, pl.ds(at, width)], end).astype(F32)
        return first, last

    @pl.when(g == 0)
    def _():
        first, last = spans(pl.multiple_of(y * COLS, COLS), COLS)
        day = day_of(lax.broadcasted_iota(jnp.int32, (SPAN, COLS), 0), tm).astype(F32)
        live = (day >= first) & (day < last)
        value = jnp.where(live, all_ref[y], 0.0)
        high_r[...], low_r[...] = split(value)
        live_r[...] = live.astype(F32).astype(BF16)
        sq_high_r[...], sq_low_r[...] = split(value * value)

    first, last = spans(pl.multiple_of(g * ROWS, ROWS), ROWS)
    first_t = jnp.broadcast_to(first, (128, ROWS)).T
    last_t = jnp.broadcast_to(last, (128, ROWS)).T
    raw = all_ref[g // 2, :, pl.ds(pl.multiple_of((g % 2) * ROWS, ROWS), ROWS)]
    day = day_of(lax.broadcasted_iota(jnp.int32, (ROWS, SPAN), 1), tm).astype(F32)
    wide = jnp.concatenate([first_t, first_t], axis=1), jnp.concatenate([last_t, last_t], axis=1)
    live = (day >= wide[0]) & (day < wide[1])
    value = jnp.where(live, raw.T, 0.0)
    high, low = split(value)
    sq_high, sq_low = split(value * value)
    live = live.astype(F32).astype(BF16)
    own_first, own_last = spans(pl.multiple_of(y * COLS, COLS), COLS)
    for n in range(0, COLS, TILE):
        at = slice(n, n + TILE)
        high_o, low_o, live_o = high_r[:, at], low_r[:, at], live_r[:, at]
        cross = dot(high, high_o) + dot(low, high_o) + dot(high, low_o)
        sum_l = dot(high, live_o) + dot(low, live_o)
        square_l = dot(sq_high, live_o) + dot(sq_low, live_o)
        sum_r = dot(live, high_o) + dot(live, low_o)
        square_r = dot(live, sq_high_r[:, at]) + dot(live, sq_low_r[:, at])
        pairs = jnp.minimum(wide[1], own_last[:, at]) - jnp.maximum(wide[0], own_first[:, at])
        pairs = jnp.maximum(pairs, 1.0)
        covariance = pairs * cross - sum_l * sum_r
        var_l = jnp.maximum(pairs * square_l - sum_l * sum_l, pairs)
        var_r = jnp.maximum(pairs * square_r - sum_r * sum_r, pairs)
        out_ref[:, at] = covariance * lax.rsqrt(var_l * var_r)


def correlated(windows, listed_from, listed_until, whole):
    full = lambda *shape: pl.BlockSpec(shape, lambda g: (0,) * len(shape))
    return pl.pallas_call(
        correlate_kernel,
        grid=(ASSETS // ROWS,),
        out_shape=jax.ShapeDtypeStruct((ASSETS, COLS), F32),
        in_specs=[
            pl.BlockSpec(memory_space=pltpu.SMEM),
            full(1, ASSETS),
            full(1, ASSETS),
            full(NY, SPAN, COLS),
        ],
        out_specs=pl.BlockSpec((ROWS, COLS), lambda g: (g, 0)),
        scratch_shapes=[pltpu.VMEM((SPAN, COLS), BF16)] * 5,
        compiler_params=pltpu.CompilerParams(dimension_semantics=("arbitrary",)),
    )(windows, listed_from[None], listed_until[None], whole)


def on_device(returns, windows, listed_from, listed_until):
    whole = gathered(returns).reshape(NY, SPAN, COLS)
    return correlated(windows, listed_from, listed_until, whole)[None]


def solution(mesh):
    placed = (P("tm", "asset"), P("tm"), P(), P())
    return jax.shard_map(
        on_device, mesh=mesh, in_specs=placed, out_specs=P("tm", None, "asset"), check_vma=False
    )
```

```python
import functools

import jax
import jax.numpy as jnp
from jax import lax
from jax.experimental import pallas as pl
from jax.experimental.pallas import tpu as pltpu
from jax.sharding import PartitionSpec as P

MESH = pl.DeviceIdType.MESH
F32, BF16 = jnp.float32, jnp.bfloat16
NZ, NX, NY = 8, 4, 4
GROUP, HALF, SPAN = 16, 8, 256
COLS, ASSETS = 512, 2048

Z_SEM = 0
YS_SEM = Z_SEM + 4
YSR_SEM = YS_SEM + 12
XA_SEM = YSR_SEM + 6
XAR_SEM = XA_SEM + 4
XB_SEM = XAR_SEM + 2
XBR_SEM = XB_SEM + 16
YA_SEM = XBR_SEM + 8
YAR_SEM = YA_SEM + 6
D_SEM = YAR_SEM + 6
E_SEM = D_SEM + 4
N_SEM = E_SEM + 4
DIRECT = frozenset({"ys", "ya", "xA", "xB"})


def gather_kernel(returns_ref, all_ref, back2, extra, ss, rs, local_sem):
    tm, y = lax.axis_index("tm"), lax.axis_index("asset")
    z, x, c = tm // 8, (tm // 2) % 4, tm % 2

    def dev(dz=0, dx=0, dy=0, dc=0):
        return (
            ((z + dz) % NZ) * 8 + ((x + dx) % NX) * 2 + (c + dc) % 2,
            (y + dy) % NY,
        )

    partner = dev(dc=1)

    def copy(src, dst, i, to):
        return pltpu.make_async_remote_copy(
            src_ref=src, dst_ref=dst, send_sem=ss.at[i], recv_sem=rs.at[i], device_id=to, device_id_type=MESH
        )

    def received(dst, i):
        copy(dst, dst, i, partner).wait_recv()

    def send(src, dst, i, to):
        copy(src, dst, i, to).start()

    def origin_block(h, at, k):
        return all_ref.at[at, c, h, x, k] if k < 2 else back2.at[h, at]

    loads = [
        pltpu.make_async_copy(returns_ref.at[pl.ds(h * HALF, HALF)], origin_block(h, y, 0), local_sem.at[h])
        for h in (0, 1)
    ]
    for load in loads:
        load.start()
    barrier = pltpu.get_barrier_semaphore()

    def greet(peer):
        pl.semaphore_signal(barrier, inc=1, device_id=peer, device_id_type=MESH)

    flat = [dev(dx=1), dev(dx=-1), dev(dy=1), dev(dy=-1), partner]
    if DIRECT & {"xA", "xB"}:
        flat.append(dev(dx=2))
    if DIRECT & {"ys", "ya"}:
        flat.append(dev(dy=2))
    for k in (1, 2):
        pl.when(z >= k)(functools.partial(greet, dev(dz=-k)))
    for peer in flat:
        greet(peer)
    pl.semaphore_wait(barrier, len(flat) + jnp.minimum(NZ - 1 - z, 2))
    for load in loads:
        load.wait()

    step = (1, -1)

    def ring_x(dx):
        return (x + dx) % NX

    def z_send(h, k):
        @pl.when(z + k < NZ)
        def _():
            send(origin_block(h, y, 0), origin_block(h, y, k), Z_SEM + h * 2 + k - 1, dev(dz=k))

    def z_wait(k):
        @pl.when(z >= k)
        def _():
            for h in (0, 1):
                received(origin_block(h, y, k), Z_SEM + h * 2 + k - 1)

    def ys_send(k):
        for h in (0, 1):
            block = origin_block(h, y, k)
            for d in (0, 1):
                send(block, block, YS_SEM + h * 6 + k * 2 + d, dev(dy=step[d]))
            if "ys" in DIRECT:
                send(block, block, YSR_SEM + h * 3 + k, dev(dy=2))

    def ys_wait(k):
        for h in (0, 1):
            for d in (0, 1):
                block = origin_block(h, (y - step[d]) % NY, k)
                received(block, YS_SEM + h * 6 + k * 2 + d)
                if (h + k) % 2 == d and "ys" not in DIRECT:
                    send(block, block, YSR_SEM + h * 3 + k, dev(dy=step[d]))

    def ysr_wait(k):
        for h in (0, 1):
            received(origin_block(h, (y + 2) % NY, k), YSR_SEM + h * 3 + k)

    def x_send(h, j, k):
        direct = "xAxB"[h * 2 : h * 2 + 2] in DIRECT
        base, relay = (XA_SEM, XAR_SEM) if h == 0 else (XB_SEM + j * 4, XBR_SEM + j * 2)
        at = (y + j) % NY
        for d in (0, 1, 2)[: 2 + direct]:
            dx = (1, -1, 2)[d]
            up = ring_x(dx) > x

            def go(slot, d=d, dx=dx):
                sem = relay + slot if d == 2 else base + d * 2 + slot
                send(origin_block(h, at, k), all_ref.at[at, c, h, x, slot], sem, dev(dx=dx))

            if k == 1:
                go(up.astype(jnp.int32))
            elif k == 0:
                pl.when(up)(functools.partial(go, 0))
            else:
                pl.when(jnp.logical_not(up))(functools.partial(go, 1))

    def x_wait(h, j):
        direct = "xAxB"[h * 2 : h * 2 + 2] in DIRECT
        base, relay = (XA_SEM, XAR_SEM) if h == 0 else (XB_SEM + j * 4, XBR_SEM + j * 2)
        at = (y + j) % NY
        first = (0, 1) if direct else (jnp.where(x == 3, 1, 0), jnp.where(x == 0, 0, 1))
        for d in (0, 1):
            block = all_ref.at[at, c, h, ring_x(-step[d]), first[d]]
            received(block, base + d * 2 + first[d])
            if not direct:
                send(block, all_ref.at[at, c, h, ring_x(-step[d]), d], relay + d, dev(dx=step[d]))
        for d in (0, 1):
            received(all_ref.at[at, c, h, ring_x(-step[d]), 1 - first[d]], base + d * 2 + 1 - first[d])

    def xr_wait(h, j):
        relay = XAR_SEM if h == 0 else XBR_SEM + j * 2
        for d in (0, 1):
            received(all_ref.at[(y + j) % NY, c, h, ring_x(2), d], relay + d)

    def ya_send(dist):
        view = all_ref.at[y, c, 0, ring_x(-dist)]
        for d in (0, 1):
            send(view, view, YA_SEM + (dist - 1) * 2 + d, dev(dy=step[d]))
        if "ya" in DIRECT:
            for d in (0, 1):
                send(view.at[d], view.at[d], YAR_SEM + (dist - 1) * 2 + d, dev(dy=2))

    def ya_wait(dist):
        for d in (0, 1):
            view = all_ref.at[(y - step[d]) % NY, c, 0, ring_x(-dist)]
            received(view, YA_SEM + (dist - 1) * 2 + d)
            if "ya" not in DIRECT:
                send(view.at[d], view.at[d], YAR_SEM + (dist - 1) * 2 + d, dev(dy=step[d]))

    def yar_wait(dist):
        for d in (0, 1):
            received(all_ref.at[(y + 2) % NY, c, 0, ring_x(-dist), d], YAR_SEM + (dist - 1) * 2 + d)

    def to_partner(j):
        at = (y + j) % NY
        send(all_ref.at[at, c], all_ref.at[at, c], D_SEM + j, partner)

        @pl.when(c == 1)
        def _():
            send(back2.at[:, at], extra.at[:, at], E_SEM + j, partner)

    def from_partner(j):
        at = (y + j) % NY
        received(all_ref.at[at, 1 - c], D_SEM + j)

        @pl.when(c == 0)
        def _():
            received(extra.at[:, at], E_SEM + j)
            all_ref[at, 1, :, x, 0] = extra[:, at]

    for k in (1, 2):
        for h in (0, 1):
            z_send(h, k)
    ys_send(0)
    x_send(0, 0, 0)
    x_send(1, 0, 0)
    ys_wait(0)
    x_send(1, 1, 0)
    x_send(1, 3, 0)
    z_wait(1)
    x_send(0, 0, 1)
    ys_send(1)
    x_send(1, 0, 1)
    ysr_wait(0)
    x_send(1, 2, 0)
    z_wait(2)
    x_send(0, 0, 2)
    ys_send(2)
    x_send(1, 0, 2)
    ys_wait(1)
    x_send(1, 1, 1)
    x_send(1, 3, 1)
    x_wait(0, 0)
    ya_send(1)
    ya_send(3)
    x_wait(1, 0)
    ysr_wait(1)
    x_send(1, 2, 1)
    ys_wait(2)
    x_send(1, 1, 2)
    x_send(1, 3, 2)
    xr_wait(0, 0)
    ya_send(2)
    ysr_wait(2)
    x_send(1, 2, 2)
    xr_wait(1, 0)
    to_partner(0)
    ya_wait(1)
    ya_wait(3)
    x_wait(1, 1)
    x_wait(1, 3)
    x_wait(1, 2)
    ya_wait(2)
    xr_wait(1, 1)
    to_partner(1)
    xr_wait(1, 3)
    to_partner(3)
    xr_wait(1, 2)
    for dist in (1, 3, 2):
        yar_wait(dist)
    to_partner(2)
    for j in (0, 1, 3, 2):
        from_partner(j)

    block, two, many = back2.at[0, 0], all_ref.at[0, 0, 0, 0], all_ref.at[0, 0]
    for i in range(E_SEM):
        view = many if i >= D_SEM else two if YA_SEM <= i < YAR_SEM else block
        done = copy(view, view, i, partner).wait_send
        if i < YS_SEM:
            pl.when(z + 1 + i % 2 < NZ)(done)
        else:
            done()

    @pl.when(c == 1)
    def _():
        for j in range(4):
            copy(back2.at[:, 0], extra.at[:, 0], E_SEM + j, partner).wait_send()


def gathered(returns):
    return pl.pallas_call(
        gather_kernel,
        out_shape=jax.ShapeDtypeStruct((NY, 2, 2, NX, 2, HALF, COLS), F32),
        in_specs=[pl.BlockSpec(memory_space=pltpu.HBM)],
        out_specs=pl.BlockSpec(memory_space=pltpu.VMEM),
        scratch_shapes=[
            pltpu.VMEM((2, NY, HALF, COLS), F32),
            pltpu.VMEM((2, NY, HALF, COLS), F32),
            pltpu.SemaphoreType.DMA((N_SEM,)),
            pltpu.SemaphoreType.DMA((N_SEM,)),
            pltpu.SemaphoreType.DMA((2,)),
        ],
        compiler_params=pltpu.CompilerParams(collective_id=0, has_side_effects=True, vmem_limit_bytes=8 << 20),
    )(returns)


def day_of(row, tm):
    core, half, at, slot, day = row // 128, (row // 64) % 2, (row // 16) % 4, (row // 8) % 2, row % 8
    place = at * 2 + core
    later = (at > (tm // 2) % 4).astype(jnp.int32)
    back = jnp.where((place == tm % 8 + 1) & (core == 1), 2 - slot, slot + later)
    return ((tm // 8 - back) * 8 + place) * GROUP + half * HALF + day


def split(value):
    high = value.astype(BF16)
    return high, (value - high.astype(F32)).astype(BF16)


def dot(left, right):
    return jnp.dot(left, right, preferred_element_type=F32)


ROWS = 256
TILE = 256


def correlate_kernel(windows_ref, from_ref, until_ref, all_ref, out_ref, high_r, low_r, live_r, sq_high_r, sq_low_r):
    tm, y = lax.axis_index("tm"), lax.axis_index("asset")
    g = pl.program_id(0)
    end = (tm + 1) * GROUP
    begin = jnp.maximum(end - windows_ref[0], 0)

    def spans(at, width):
        first = jnp.maximum(from_ref[:, pl.ds(at, width)], begin).astype(F32)
        last = jnp.minimum(until_ref[:, pl.ds(at, width)], end).astype(F32)
        return first, last

    @pl.when(g == 0)
    def _():
        first, last = spans(pl.multiple_of(y * COLS, COLS), COLS)
        day = day_of(lax.broadcasted_iota(jnp.int32, (SPAN, COLS), 0), tm).astype(F32)
        live = (day >= first) & (day < last)
        value = jnp.where(live, all_ref[y], 0.0)
        high_r[...], low_r[...] = split(value)
        live_r[...] = live.astype(F32).astype(BF16)
        sq_high_r[...], sq_low_r[...] = split(value * value)

    first, last = spans(pl.multiple_of(g * ROWS, ROWS), ROWS)
    first_t = jnp.broadcast_to(first, (128, ROWS)).T
    last_t = jnp.broadcast_to(last, (128, ROWS)).T
    raw = all_ref[g // 2, :, pl.ds(pl.multiple_of((g % 2) * ROWS, ROWS), ROWS)]
    day = day_of(lax.broadcasted_iota(jnp.int32, (ROWS, SPAN), 1), tm).astype(F32)
    wide = jnp.concatenate([first_t, first_t], axis=1), jnp.concatenate([last_t, last_t], axis=1)
    live = (day >= wide[0]) & (day < wide[1])
    value = jnp.where(live, raw.T, 0.0)
    high, low = split(value)
    sq_high, sq_low = split(value * value)
    live = live.astype(F32).astype(BF16)
    own_first, own_last = spans(pl.multiple_of(y * COLS, COLS), COLS)
    for n in range(0, COLS, TILE):
        at = slice(n, n + TILE)
        high_o, low_o, live_o = high_r[:, at], low_r[:, at], live_r[:, at]
        cross = dot(high, high_o) + dot(low, high_o) + dot(high, low_o)
        sum_l = dot(high, live_o) + dot(low, live_o)
        square_l = dot(sq_high, live_o) + dot(sq_low, live_o)
        sum_r = dot(live, high_o) + dot(live, low_o)
        square_r = dot(live, sq_high_r[:, at]) + dot(live, sq_low_r[:, at])
        pairs = jnp.minimum(wide[1], own_last[:, at]) - jnp.maximum(wide[0], own_first[:, at])
        pairs = jnp.maximum(pairs, 1.0)
        covariance = pairs * cross - sum_l * sum_r
        var_l = jnp.maximum(pairs * square_l - sum_l * sum_l, pairs)
        var_r = jnp.maximum(pairs * square_r - sum_r * sum_r, pairs)
        out_ref[:, at] = covariance * lax.rsqrt(var_l * var_r)


def correlated(windows, listed_from, listed_until, whole):
    full = lambda *shape: pl.BlockSpec(shape, lambda g: (0,) * len(shape))
    return pl.pallas_call(
        correlate_kernel,
        grid=(ASSETS // ROWS,),
        out_shape=jax.ShapeDtypeStruct((ASSETS, COLS), F32),
        in_specs=[
            pl.BlockSpec(memory_space=pltpu.SMEM),
            full(1, ASSETS),
            full(1, ASSETS),
            full(NY, SPAN, COLS),
        ],
        out_specs=pl.BlockSpec((ROWS, COLS), lambda g: (g, 0)),
        scratch_shapes=[pltpu.VMEM((SPAN, COLS), BF16)] * 5,
        compiler_params=pltpu.CompilerParams(dimension_semantics=("arbitrary",), vmem_limit_bytes=16 << 20),
    )(windows, listed_from[None], listed_until[None], whole)


def on_device(returns, windows, listed_from, listed_until):
    whole = gathered(returns).reshape(NY, SPAN, COLS)
    return correlated(windows, listed_from, listed_until, whole)[None]


def solution(mesh):
    placed = (P("tm", "asset"), P("tm"), P(), P())
    return jax.shard_map(
        on_device, mesh=mesh, in_specs=placed, out_specs=P("tm", None, "asset"), check_vma=False
    )
```

```python
import functools

import jax
import jax.numpy as jnp
from jax import lax
from jax.experimental import pallas as pl
from jax.experimental.pallas import tpu as pltpu
from jax.sharding import PartitionSpec as P

MESH = pl.DeviceIdType.MESH
F32, BF16 = jnp.float32, jnp.bfloat16
NZ, NX, NY = 8, 4, 4
GROUP, HALF, SPAN = 16, 8, 256
COLS, ASSETS = 512, 2048

Z_SEM = 0
YS_SEM = Z_SEM + 4
YSR_SEM = YS_SEM + 12
XA_SEM = YSR_SEM + 6
XAR_SEM = XA_SEM + 4
XB_SEM = XAR_SEM + 2
XBR_SEM = XB_SEM + 16
YA_SEM = XBR_SEM + 8
D_SEM = YA_SEM + 18
E_SEM = D_SEM + 4
N_SEM = E_SEM + 4


def gather_kernel(
    returns_ref,
    windows_ref,
    from_hbm,
    until_hbm,
    all_ref,
    own_ref,
    out_ref,
    from_ref,
    until_ref,
    back2,
    extra,
    wide_ref,
    ss,
    rs,
    local_sem,
):
    tm, y = lax.axis_index("tm"), lax.axis_index("asset")
    z, x, c = tm // 8, (tm // 2) % 4, tm % 2

    def dev(dz=0, dx=0, dy=0, dc=0):
        return (
            ((z + dz) % NZ) * 8 + ((x + dx) % NX) * 2 + (c + dc) % 2,
            (y + dy) % NY,
        )

    partner = dev(dc=1)

    def copy(src, dst, i, to):
        return pltpu.make_async_remote_copy(
            src_ref=src, dst_ref=dst, send_sem=ss.at[i], recv_sem=rs.at[i], device_id=to, device_id_type=MESH
        )

    def received(dst, i):
        copy(dst, dst, i, partner).wait_recv()

    def send(src, dst, i, to):
        copy(src, dst, i, to).start()

    def origin_block(h, at, k):
        return all_ref.at[at, c, h, x, k] if k < 2 else back2.at[h, at]

    loads = [
        pltpu.make_async_copy(returns_ref.at[pl.ds(h * HALF, HALF)], origin_block(h, y, 0), local_sem.at[h])
        for h in (0, 1)
    ]
    lists = [
        pltpu.make_async_copy(from_hbm, from_ref, local_sem.at[2]),
        pltpu.make_async_copy(until_hbm, until_ref, local_sem.at[3]),
    ]
    for load in loads + lists:
        load.start()
    barrier = pltpu.get_barrier_semaphore()

    def greet(peer):
        pl.semaphore_signal(barrier, inc=1, device_id=peer, device_id_type=MESH)

    flat = [dev(dx=1), dev(dx=-1), dev(dx=2), dev(dy=1), dev(dy=-1), dev(dy=2), partner]
    for k in (1, 2):
        pl.when(z >= k)(functools.partial(greet, dev(dz=-k)))
    for peer in flat:
        greet(peer)
    pl.semaphore_wait(barrier, len(flat) + jnp.minimum(NZ - 1 - z, 2))
    for load in loads:
        load.wait()

    step = (1, -1)

    def ring_x(dx):
        return (x + dx) % NX

    def z_send(h, k):
        @pl.when(z + k < NZ)
        def _():
            send(origin_block(h, y, 0), origin_block(h, y, k), Z_SEM + h * 2 + k - 1, dev(dz=k))

    def z_wait(k):
        @pl.when(z >= k)
        def _():
            for h in (0, 1):
                received(origin_block(h, y, k), Z_SEM + h * 2 + k - 1)

    def ys_send(k):
        for h in (0, 1):
            block = origin_block(h, y, k)
            for d in (0, 1):
                send(block, block, YS_SEM + h * 6 + k * 2 + d, dev(dy=step[d]))
            send(block, block, YSR_SEM + h * 3 + k, dev(dy=2))

    def ys_wait(k):
        for h in (1, 0):
            for d in (0, 1):
                received(origin_block(h, (y - step[d]) % NY, k), YS_SEM + h * 6 + k * 2 + d)

    def ysr_wait(k):
        for h in (1, 0):
            received(origin_block(h, (y + 2) % NY, k), YSR_SEM + h * 3 + k)

    def x_sem(h, j, d, slot):
        near, far = (XA_SEM, XAR_SEM) if h == 0 else (XB_SEM + j * 4, XBR_SEM + j * 2)
        return far + slot if d == 2 else near + d * 2 + slot

    def with_slot(k, up, go):
        if k == 1:
            go(up.astype(jnp.int32))
        elif k == 0:
            pl.when(up)(functools.partial(go, 0))
        else:
            pl.when(jnp.logical_not(up))(functools.partial(go, 1))

    def x_send(h, j, k):
        at = (y + j) % NY
        for d, dx in ((2, 2), (0, 1), (1, -1)):

            def go(slot, d=d, dx=dx):
                send(origin_block(h, at, k), all_ref.at[at, c, h, x, slot], x_sem(h, j, d, slot), dev(dx=dx))

            with_slot(k, ring_x(dx) > x, go)

    def x_wait(h, j, k, far, then=None):
        at = (y + j) % NY
        for d, dx in ((2, 2),) if far else ((0, 1), (1, -1)):

            def go(slot, d=d, dx=dx):
                received(all_ref.at[at, c, h, ring_x(-dx), slot], x_sem(h, j, d, slot))
                if then is not None:
                    then(dx % NX, slot)

            with_slot(k, ring_x(-dx) < x, go)

    def ya_send(dist, slot):
        view = all_ref.at[y, c, 0, ring_x(-dist), slot]
        for dy in (2, 1, 3):
            send(view, view, YA_SEM + (dist - 1) * 6 + (dy - 1) * 2 + slot, dev(dy=dy))

    def ya_wait(j):
        for dist in (1, 3, 2):
            for slot in (0, 1):
                view = all_ref.at[(y + j) % NY, c, 0, ring_x(-dist), slot]
                received(view, YA_SEM + (dist - 1) * 6 + (3 - j) * 2 + slot)

    def x_all(h, j, ks=(0, 1, 2)):
        for k in ks:
            for far in (False, True):
                x_wait(h, j, k, far)

    def to_partner(j):
        at = (y + j) % NY
        send(all_ref.at[at, c], all_ref.at[at, c], D_SEM + j, partner)

        @pl.when(c == 1)
        def _():
            send(back2.at[:, at], extra.at[:, at], E_SEM + j, partner)

    def from_partner(j):
        at = (y + j) % NY
        received(all_ref.at[at, 1 - c], D_SEM + j)

        @pl.when(c == 0)
        def _():
            received(extra.at[:, at], E_SEM + j)
            all_ref[at, 1, :, x, 0] = extra[:, at]

    for k in (2, 1):
        for h in (1, 0):
            z_send(h, k)
    ys_send(0)
    x_send(0, 0, 0)
    x_send(1, 0, 0)
    ys_wait(0)
    x_send(1, 1, 0)
    x_send(1, 3, 0)
    z_wait(1)
    x_send(0, 0, 1)
    ys_send(1)
    x_send(1, 0, 1)
    ysr_wait(0)
    x_send(1, 2, 0)
    z_wait(2)
    x_send(0, 0, 2)
    ys_send(2)
    x_send(1, 0, 2)
    x_wait(0, 0, 0, False, ya_send)
    x_wait(0, 0, 0, True, ya_send)
    ys_wait(1)
    x_send(1, 1, 1)
    x_send(1, 3, 1)
    x_wait(0, 0, 1, False, ya_send)
    ysr_wait(1)
    x_send(1, 2, 1)
    x_wait(0, 0, 1, True, ya_send)
    ys_wait(2)
    x_send(1, 1, 2)
    x_send(1, 3, 2)
    x_wait(0, 0, 2, False, ya_send)
    ysr_wait(2)
    x_send(1, 2, 2)
    x_wait(0, 0, 2, True, ya_send)
    x_all(1, 0)
    to_partner(0)
    from_partner(0)

    for load in lists:
        load.wait()
    spans = spans_of(windows_ref, from_ref, until_ref, tm)
    own_spans = spans(pl.multiple_of(y * COLS, COLS), COLS)
    prepare_own(all_ref[y].reshape(SPAN, COLS), own_spans, tm, own_ref)

    def own_rows(i):
        at = pl.multiple_of(y * COLS + i * ROWS, ROWS)
        raw = all_ref[y].reshape(SPAN, COLS)[:, i * ROWS : (i + 1) * ROWS]
        rows = prepare(raw, spans(at, ROWS), tm, wide_ref)
        correlate(wide_ref, rows, own_ref, own_spans, out_ref.at[pl.ds(i * ROWS, ROWS)])

    own_rows(0)
    for j in (1, 3, 2):
        x_all(1, j)
        ya_wait(j)
        to_partner(j)
    own_rows(1)
    for j in (1, 3, 2):
        from_partner(j)

    block, many = back2.at[0, 0], all_ref.at[0, 0]
    for i in range(E_SEM):
        view = many if i >= D_SEM else block
        done = copy(view, view, i, partner).wait_send
        if i < YS_SEM:
            pl.when(z + 1 + i % 2 < NZ)(done)
        else:
            done()

    @pl.when(c == 1)
    def _():
        for j in range(4):
            copy(back2.at[:, 0], extra.at[:, 0], E_SEM + j, partner).wait_send()


ROWS = 256
TILE = 256


def day_of(row, tm):
    core, half, at, slot, day = row // 128, (row // 64) % 2, (row // 16) % 4, (row // 8) % 2, row % 8
    place = at * 2 + core
    later = (at > (tm // 2) % 4).astype(jnp.int32)
    back = jnp.where((place == tm % 8 + 1) & (core == 1), 2 - slot, slot + later)
    return ((tm // 8 - back) * 8 + place) * GROUP + half * HALF + day


def split(value):
    high = value.astype(BF16)
    return high, (value - high.astype(F32)).astype(BF16)


def dot(left, right):
    return jnp.dot(left, right, preferred_element_type=F32)


def spans_of(windows_ref, from_ref, until_ref, tm):
    end = (tm + 1) * GROUP
    begin = jnp.maximum(end - windows_ref[0], 0)

    def spans(at, width):
        first = jnp.maximum(from_ref[:, pl.ds(at, width)], begin).astype(F32)
        last = jnp.minimum(until_ref[:, pl.ds(at, width)], end).astype(F32)
        return first, last

    return spans


def terms(day, first, last, raw, out_ref):
    live = (day >= first) & (day < last)
    value = jnp.where(live, raw, 0.0)
    out_ref[0] = live.astype(F32).astype(BF16)
    out_ref[1], out_ref[2] = split(value)
    out_ref[3], out_ref[4] = split(value * value)


def prepare_own(raw, spans, tm, own_ref):
    day = day_of(lax.broadcasted_iota(jnp.int32, (SPAN, 128), 0), tm).astype(F32)
    for n in range(0, COLS, 128):
        at = slice(n, n + 128)
        terms(day, spans[0][:, at], spans[1][:, at], raw[:, at], own_ref.at[:, :, pl.ds(n, 128)])


def prepare(raw, spans, tm, wide_ref):
    day = day_of(lax.broadcasted_iota(jnp.int32, (1, SPAN), 1), tm).astype(F32)
    first, last = (jnp.broadcast_to(span, (128, ROWS)).T for span in spans)
    for n in range(0, SPAN, 128):
        terms(day[:, n : n + 128], first, last, raw[n : n + 128].T, wide_ref.at[:, :, pl.ds(n, 128)])
    return first, last


def correlate(wide, rows, own_ref, own_spans, out_ref):
    first, last = rows
    live, high, low, sq_high, sq_low = (wide[i] for i in range(5))
    for n in range(0, COLS, TILE):
        at = slice(n, n + TILE)
        live_o, high_o, low_o, sq_high_o, sq_low_o = (own_ref[i, :, at] for i in range(5))
        cross = dot(high, high_o) + dot(low, high_o) + dot(high, low_o)
        sum_l = dot(high, live_o) + dot(low, live_o)
        square_l = dot(sq_high, live_o) + dot(sq_low, live_o)
        sum_r = dot(live, high_o) + dot(live, low_o)
        square_r = dot(live, sq_high_o) + dot(live, sq_low_o)
        pairs = jnp.concatenate(
            [
                jnp.minimum(last, own_spans[1][:, m : m + 128]) - jnp.maximum(first, own_spans[0][:, m : m + 128])
                for m in range(n, n + TILE, 128)
            ],
            axis=1,
        )
        pairs = jnp.maximum(pairs, 1.0)
        covariance = pairs * cross - sum_l * sum_r
        var_l = jnp.maximum(pairs * square_l - sum_l * sum_l, pairs)
        var_r = jnp.maximum(pairs * square_r - sum_r * sum_r, pairs)
        out_ref[:, at] = covariance * lax.rsqrt(var_l * var_r)


def gathered(returns, windows, listed_from, listed_until):
    vmem, smem, hbm = (pl.BlockSpec(memory_space=space) for space in (pltpu.VMEM, pltpu.SMEM, pltpu.HBM))
    returns, listed_from, listed_until = (
        pltpu.with_memory_space_constraint(array, pltpu.HBM) for array in (returns, listed_from, listed_until)
    )
    return pl.pallas_call(
        gather_kernel,
        out_shape=[
            jax.ShapeDtypeStruct((NY, 2, 2, NX, 2, HALF, COLS), F32),
            jax.ShapeDtypeStruct((5, SPAN, COLS), BF16),
            jax.ShapeDtypeStruct((COLS, COLS), F32),
            jax.ShapeDtypeStruct((1, ASSETS), jnp.int32),
            jax.ShapeDtypeStruct((1, ASSETS), jnp.int32),
        ],
        in_specs=[hbm, smem, hbm, hbm],
        out_specs=[vmem] * 5,
        scratch_shapes=[
            pltpu.VMEM((2, NY, HALF, COLS), F32),
            pltpu.VMEM((2, NY, HALF, COLS), F32),
            pltpu.VMEM((5, ROWS, SPAN), BF16),
            pltpu.SemaphoreType.DMA((N_SEM,)),
            pltpu.SemaphoreType.DMA((N_SEM,)),
            pltpu.SemaphoreType.DMA((4,)),
        ],
        compiler_params=pltpu.CompilerParams(collective_id=0, has_side_effects=True, vmem_limit_bytes=16 << 20),
    )(returns, windows, listed_from, listed_until)


ORDER = (1, 3, 2)


def rest_kernel(windows_ref, all_ref, own_ref, done_ref, from_ref, until_ref, out_ref, wide_a, wide_b, result, sems):
    tm, y = lax.axis_index("tm"), lax.axis_index("asset")
    spans = spans_of(windows_ref, from_ref, until_ref, tm)
    own_spans = spans(pl.multiple_of(y * COLS, COLS), COLS)
    copies = [pltpu.make_async_copy(done_ref, out_ref.at[pl.ds(pl.multiple_of(y * COLS, COLS), COLS)], sems.at[6])]
    copies[0].start()
    wides = wide_a, wide_b

    def place(i):
        at = (y + ORDER[i // 2]) % NY
        return at, pl.multiple_of(at * COLS + (i % 2) * ROWS, ROWS)

    def ready(i):
        at, row = place(i)
        raw = all_ref[at].reshape(SPAN, COLS)[:, (i % 2) * ROWS : (i % 2 + 1) * ROWS]
        return prepare(raw, spans(row, ROWS), tm, wides[i % 2])

    rows = ready(0)
    for i in range(6):
        now = rows
        if i < 5:
            rows = ready(i + 1)
        correlate(wides[i % 2], now, own_ref, own_spans, result.at[i])
        copies.append(pltpu.make_async_copy(result.at[i], out_ref.at[pl.ds(place(i)[1], ROWS)], sems.at[i]))
        copies[-1].start()
    for copy in copies:
        copy.wait()


def completed(windows, whole, own, done, listed_from, listed_until):
    vmem, smem = pl.BlockSpec(memory_space=pltpu.VMEM), pl.BlockSpec(memory_space=pltpu.SMEM)
    return pl.pallas_call(
        rest_kernel,
        out_shape=jax.ShapeDtypeStruct((ASSETS, COLS), F32),
        in_specs=[smem, vmem, vmem, vmem, vmem, vmem],
        out_specs=pl.BlockSpec(memory_space=pltpu.HBM),
        scratch_shapes=[pltpu.VMEM((5, ROWS, SPAN), BF16)] * 2
        + [pltpu.VMEM((6, ROWS, COLS), F32), pltpu.SemaphoreType.DMA((7,))],
        compiler_params=pltpu.CompilerParams(vmem_limit_bytes=20 << 20),
    )(windows, whole, own, done, listed_from, listed_until)


def on_device(returns, windows, listed_from, listed_until):
    return completed(windows, *gathered(returns, windows, listed_from[None], listed_until[None]))[None]


def solution(mesh):
    placed = (P("tm", "asset"), P("tm"), P(), P())
    return jax.shard_map(
        on_device, mesh=mesh, in_specs=placed, out_specs=P("tm", None, "asset"), check_vma=False
    )
```

```python
import functools

import jax
import jax.numpy as jnp
from jax import lax
from jax.experimental import pallas as pl
from jax.experimental.pallas import tpu as pltpu
from jax.sharding import PartitionSpec as P

MESH = pl.DeviceIdType.MESH
F32, BF16 = jnp.float32, jnp.bfloat16
NZ, NX, NY = 8, 4, 4
GROUP, HALF, SPAN = 16, 8, 256
COLS, ASSETS = 512, 2048

Z_SEM = 0
YS_SEM = Z_SEM + 4
YSR_SEM = YS_SEM + 12
XA_SEM = YSR_SEM + 6
XAR_SEM = XA_SEM + 4
XB_SEM = XAR_SEM + 2
XBR_SEM = XB_SEM + 16
YA_SEM = XBR_SEM + 8
D_SEM = YA_SEM + 18
E_SEM = D_SEM + 4
N_SEM = E_SEM + 4


def gather_kernel(
    returns_ref,
    windows_ref,
    from_hbm,
    until_hbm,
    all_ref,
    own_ref,
    out_ref,
    from_ref,
    until_ref,
    back2,
    extra,
    wide_ref,
    ss,
    rs,
    local_sem,
):
    tm, y = lax.axis_index("tm"), lax.axis_index("asset")
    z, x, c = tm // 8, (tm // 2) % 4, tm % 2

    def dev(dz=0, dx=0, dy=0, dc=0):
        return (
            ((z + dz) % NZ) * 8 + ((x + dx) % NX) * 2 + (c + dc) % 2,
            (y + dy) % NY,
        )

    partner = dev(dc=1)

    def copy(src, dst, i, to):
        return pltpu.make_async_remote_copy(
            src_ref=src, dst_ref=dst, send_sem=ss.at[i], recv_sem=rs.at[i], device_id=to, device_id_type=MESH
        )

    def received(dst, i):
        copy(dst, dst, i, partner).wait_recv()

    def send(src, dst, i, to):
        copy(src, dst, i, to).start()

    def origin_block(h, at, k):
        return all_ref.at[at, c, h, x, k] if k < 2 else back2.at[h, at]

    loads = [
        pltpu.make_async_copy(returns_ref.at[pl.ds(h * HALF, HALF)], origin_block(h, y, 0), local_sem.at[h])
        for h in (0, 1)
    ]
    lists = [
        pltpu.make_async_copy(from_hbm, from_ref, local_sem.at[2]),
        pltpu.make_async_copy(until_hbm, until_ref, local_sem.at[3]),
    ]
    for load in loads + lists:
        load.start()
    barrier = pltpu.get_barrier_semaphore()

    def greet(peer):
        pl.semaphore_signal(barrier, inc=1, device_id=peer, device_id_type=MESH)

    flat = [dev(dx=1), dev(dx=-1), dev(dx=2), dev(dy=1), dev(dy=-1), dev(dy=2), partner]
    for k in (1, 2):
        pl.when(z >= k)(functools.partial(greet, dev(dz=-k)))
    for peer in flat:
        greet(peer)
    pl.semaphore_wait(barrier, len(flat) + jnp.minimum(NZ - 1 - z, 2))
    for load in loads:
        load.wait()

    step = (1, -1)

    def ring_x(dx):
        return (x + dx) % NX

    def z_send(h, k):
        @pl.when(z + k < NZ)
        def _():
            send(origin_block(h, y, 0), origin_block(h, y, k), Z_SEM + h * 2 + k - 1, dev(dz=k))

    def z_wait(k):
        @pl.when(z >= k)
        def _():
            for h in (0, 1):
                received(origin_block(h, y, k), Z_SEM + h * 2 + k - 1)

    def y_sem(h, j, k):
        return YSR_SEM + h * 3 + k if j == 2 else YS_SEM + h * 6 + k * 2 + (0 if j == 3 else 1)

    def ys_send(js):
        for h in (1, 0):
            block = origin_block(h, y, 0)
            for j in js:
                send(block, block, y_sem(h, (NY - j) % NY, 0), dev(dy=j))

    def needed(h, k):
        return (z >= k) & (c == 1) if (h, k) == (0, 2) else z >= k

    def passed_on(h, k):
        here = (z >= k - 1) & (z + 1 < NZ)
        return here & (c == 1) if (h, k) == (0, 2) else here

    def ys_wait(js, k):
        for j in js:
            at = (y + j) % NY
            for h in (1, 0):

                def arrive(h=h, at=at, j=j):
                    received(origin_block(h, at, k), y_sem(h, j, k))

                arrive() if k == 0 else pl.when(needed(h, k))(arrive)

                def forward(h=h, at=at, j=j):
                    send(origin_block(h, at, k), origin_block(h, at, k + 1), y_sem(h, j, k + 1), dev(dz=1))

                if k < 2:
                    pl.when(passed_on(h, k + 1))(forward)

    def x_sem(h, j, d, slot):
        near, far = (XA_SEM, XAR_SEM) if h == 0 else (XB_SEM + j * 4, XBR_SEM + j * 2)
        return far + slot if d == 2 else near + d * 2 + slot

    def with_slot(k, up, go):
        if k == 1:
            go(up.astype(jnp.int32))
        elif k == 0:
            pl.when(up)(functools.partial(go, 0))
        else:
            pl.when(jnp.logical_not(up))(functools.partial(go, 1))

    def x_send(h, j, k):
        at = (y + j) % NY
        for d, dx in ((2, 2), (0, 1), (1, -1)):

            def go(slot, d=d, dx=dx):
                send(origin_block(h, at, k), all_ref.at[at, c, h, x, slot], x_sem(h, j, d, slot), dev(dx=dx))

            with_slot(k, ring_x(dx) > x, go)

    def x_wait(h, j, k, far, then=None):
        at = (y + j) % NY
        for d, dx in ((2, 2),) if far else ((0, 1), (1, -1)):

            def go(slot, d=d, dx=dx):
                received(all_ref.at[at, c, h, ring_x(-dx), slot], x_sem(h, j, d, slot))
                if then is not None:
                    then(dx % NX, slot)

            with_slot(k, ring_x(-dx) < x, go)

    def ya_send(dist, slot, to=(1, 3)):
        view = all_ref.at[y, c, 0, ring_x(-dist), slot]
        for dy in to:
            send(view, view, YA_SEM + (dist - 1) * 6 + (dy - 1) * 2 + slot, dev(dy=dy))

    def ya_wait(j):
        for dist in (1, 3, 2):
            for slot in (0, 1):
                view = all_ref.at[(y + j) % NY, c, 0, ring_x(-dist), slot]
                received(view, YA_SEM + (dist - 1) * 6 + (3 - j) * 2 + slot)

    def x_all(h, j, ks=(0, 1, 2)):
        for k in ks:
            for far in (False, True):
                x_wait(h, j, k, far)

    def to_partner(j):
        at = (y + j) % NY
        send(all_ref.at[at, c], all_ref.at[at, c], D_SEM + j, partner)

        @pl.when(c == 1)
        def _():
            send(back2.at[:, at], extra.at[:, at], E_SEM + j, partner)

    def from_partner(j):
        at = (y + j) % NY
        received(all_ref.at[at, 1 - c], D_SEM + j)

        @pl.when(c == 0)
        def _():
            received(extra.at[:, at], E_SEM + j)
            all_ref[at, 1, :, x, 0] = extra[:, at]

    ys_send((1, 3, 2))
    for k in (2, 1):
        for h in (1, 0):
            z_send(h, k)
    for k in (0, 1, 2):
        if k:
            z_wait(k)
        x_send(0, 0, k)
        x_send(1, 0, k)
    ys_wait((1, 3), 0)
    x_send(1, 1, 0)
    x_send(1, 3, 0)
    ys_wait((2,), 0)
    for k in (0, 1):
        x_wait(0, 0, k, False, ya_send)
        x_wait(0, 0, k, True, ya_send)
    ys_wait((1, 3), 1)
    x_send(1, 1, 1)
    x_send(1, 3, 1)
    ys_wait((2,), 1)
    x_wait(0, 0, 2, False, ya_send)
    x_wait(0, 0, 2, True, ya_send)
    ys_wait((1, 3), 2)
    x_send(1, 1, 2)
    x_send(1, 3, 2)
    for dist in (1, 3, 2):
        for slot in (0, 1):
            ya_send(dist, slot, (2,))
    x_send(1, 2, 0)
    x_send(1, 2, 1)
    ys_wait((2,), 2)
    x_send(1, 2, 2)
    x_all(1, 0)
    to_partner(0)

    for load in lists:
        load.wait()
    spans = spans_of(windows_ref, from_ref, until_ref, tm)
    own_spans = spans(pl.multiple_of(y * COLS, COLS), COLS)

    def some_rows(i):
        at, row = place_of(i, y)
        raw = all_ref[at].reshape(SPAN, COLS)[:, (i % 2) * ROWS : (i % 2 + 1) * ROWS]
        rows = prepare(raw, spans(row, ROWS), tm, wide_ref)
        correlate(wide_ref, rows, own_ref, own_spans, out_ref.at[pl.ds(i * ROWS, ROWS)])

    from_partner(0)
    prepare_own(all_ref[y].reshape(SPAN, COLS), own_spans, tm, own_ref)
    some_rows(0)
    some_rows(1)
    x_all(1, 1)
    ya_wait(1)
    to_partner(1)
    x_all(1, 3)
    ya_wait(3)
    to_partner(3)
    from_partner(1)
    some_rows(2)
    x_all(1, 2)
    ya_wait(2)
    to_partner(2)
    some_rows(3)
    from_partner(3)
    some_rows(4)
    from_partner(2)
    block, many = back2.at[0, 0], all_ref.at[0, 0]
    for i in range(E_SEM):
        view = many if i >= D_SEM else block
        done = copy(view, view, i, partner).wait_send
        if i < YS_SEM:
            pl.when(z + 1 + i % 2 < NZ)(done)
        elif i < XA_SEM:
            h, k = divmod(i - YSR_SEM, 3) if i >= YSR_SEM else divmod((i - YS_SEM) // 2, 3)
            pl.when(passed_on(h, k))(done) if k else done()
        else:
            done()

    @pl.when(c == 1)
    def _():
        for j in range(4):
            copy(back2.at[:, 0], extra.at[:, 0], E_SEM + j, partner).wait_send()


ROWS = 256
TILE = 256
ORDER = (0, 1, 3, 2)
FIRST = 5


def place_of(i, y):
    at = (y + ORDER[i // 2]) % NY
    return at, pl.multiple_of(at * COLS + (i % 2) * ROWS, ROWS)


def day_of(row, tm):
    core, half, at, slot, day = row // 128, (row // 64) % 2, (row // 16) % 4, (row // 8) % 2, row % 8
    place = at * 2 + core
    later = (at > (tm // 2) % 4).astype(jnp.int32)
    back = jnp.where((place == tm % 8 + 1) & (core == 1), 2 - slot, slot + later)
    return ((tm // 8 - back) * 8 + place) * GROUP + half * HALF + day


def split(value):
    high = value.astype(BF16)
    return high, (value - high.astype(F32)).astype(BF16)


def dot(left, right):
    return jnp.dot(left, right, preferred_element_type=F32)


def spans_of(windows_ref, from_ref, until_ref, tm):
    end = (tm + 1) * GROUP
    begin = jnp.maximum(end - windows_ref[0], 0)

    def spans(at, width):
        first = jnp.maximum(from_ref[:, pl.ds(at, width)], begin).astype(F32)
        last = jnp.minimum(until_ref[:, pl.ds(at, width)], end).astype(F32)
        return first, last

    return spans


def terms(day, first, last, raw, out_ref):
    live = (day >= first) & (day < last)
    value = jnp.where(live, raw, 0.0)
    out_ref[0] = live.astype(F32).astype(BF16)
    out_ref[1], out_ref[2] = split(value)
    out_ref[3], out_ref[4] = split(value * value)


def prepare_own(raw, spans, tm, own_ref):
    day = day_of(lax.broadcasted_iota(jnp.int32, (SPAN, 128), 0), tm).astype(F32)
    for n in range(0, COLS, 128):
        at = slice(n, n + 128)
        terms(day, spans[0][:, at], spans[1][:, at], raw[:, at], own_ref.at[:, :, pl.ds(n, 128)])


def prepare(raw, spans, tm, wide_ref):
    day = day_of(lax.broadcasted_iota(jnp.int32, (1, SPAN), 1), tm).astype(F32)
    first, last = (jnp.broadcast_to(span, (128, ROWS)).T for span in spans)
    for n in range(0, SPAN, 128):
        terms(day[:, n : n + 128], first, last, raw[n : n + 128].T, wide_ref.at[:, :, pl.ds(n, 128)])
    return first, last


def correlate(wide, rows, own_ref, own_spans, out_ref):
    first, last = rows
    live, high, low, sq_high, sq_low = (wide[i] for i in range(5))
    for n in range(0, COLS, TILE):
        at = slice(n, n + TILE)
        live_o, high_o, low_o, sq_high_o, sq_low_o = (own_ref[i, :, at] for i in range(5))
        cross = dot(high, high_o) + dot(low, high_o) + dot(high, low_o)
        sum_l = dot(high, live_o) + dot(low, live_o)
        square_l = dot(sq_high, live_o) + dot(sq_low, live_o)
        sum_r = dot(live, high_o) + dot(live, low_o)
        square_r = dot(live, sq_high_o) + dot(live, sq_low_o)
        pairs = jnp.concatenate(
            [
                jnp.minimum(last, own_spans[1][:, m : m + 128]) - jnp.maximum(first, own_spans[0][:, m : m + 128])
                for m in range(n, n + TILE, 128)
            ],
            axis=1,
        )
        pairs = jnp.maximum(pairs, 1.0)
        covariance = pairs * cross - sum_l * sum_r
        var_l = jnp.maximum(pairs * square_l - sum_l * sum_l, pairs)
        var_r = jnp.maximum(pairs * square_r - sum_r * sum_r, pairs)
        out_ref[:, at] = covariance * lax.rsqrt(var_l * var_r)


def gathered(returns, windows, listed_from, listed_until):
    vmem, smem, hbm = (pl.BlockSpec(memory_space=space) for space in (pltpu.VMEM, pltpu.SMEM, pltpu.HBM))
    returns, listed_from, listed_until = (
        pltpu.with_memory_space_constraint(array, pltpu.HBM) for array in (returns, listed_from, listed_until)
    )
    return pl.pallas_call(
        gather_kernel,
        out_shape=[
            jax.ShapeDtypeStruct((NY, 2, 2, NX, 2, HALF, COLS), F32),
            jax.ShapeDtypeStruct((5, SPAN, COLS), BF16),
            jax.ShapeDtypeStruct((FIRST * ROWS, COLS), F32),
            jax.ShapeDtypeStruct((1, ASSETS), jnp.int32),
            jax.ShapeDtypeStruct((1, ASSETS), jnp.int32),
        ],
        in_specs=[hbm, smem, hbm, hbm],
        out_specs=[vmem] * 5,
        scratch_shapes=[
            pltpu.VMEM((2, NY, HALF, COLS), F32),
            pltpu.VMEM((2, NY, HALF, COLS), F32),
            pltpu.VMEM((5, ROWS, SPAN), BF16),
            pltpu.SemaphoreType.DMA((N_SEM,)),
            pltpu.SemaphoreType.DMA((N_SEM,)),
            pltpu.SemaphoreType.DMA((4,)),
        ],
        compiler_params=pltpu.CompilerParams(collective_id=0, has_side_effects=True, vmem_limit_bytes=16 << 20),
    )(returns, windows, listed_from, listed_until)


def rest_kernel(windows_ref, all_ref, own_ref, done_ref, from_ref, until_ref, out_ref, wide_a, wide_b, result, sems):
    tm, y = lax.axis_index("tm"), lax.axis_index("asset")
    spans = spans_of(windows_ref, from_ref, until_ref, tm)
    own_spans = spans(pl.multiple_of(y * COLS, COLS), COLS)
    copies = []

    def store(src, i):
        copies.append(pltpu.make_async_copy(src, out_ref.at[pl.ds(place_of(i, y)[1], ROWS)], sems.at[i]))
        copies[-1].start()

    for i in range(FIRST):
        store(done_ref.at[pl.ds(i * ROWS, ROWS)], i)
    wides = wide_a, wide_b

    def ready(i):
        at, row = place_of(i, y)
        raw = all_ref[at].reshape(SPAN, COLS)[:, (i % 2) * ROWS : (i % 2 + 1) * ROWS]
        return prepare(raw, spans(row, ROWS), tm, wides[i % 2])

    rows = ready(FIRST)
    for i in range(FIRST, 8):
        now = rows
        if i < 7:
            rows = ready(i + 1)
        correlate(wides[i % 2], now, own_ref, own_spans, result.at[i - FIRST])
        store(result.at[i - FIRST], i)
    for copy in copies:
        copy.wait()


def completed(windows, whole, own, done, listed_from, listed_until):
    vmem, smem = pl.BlockSpec(memory_space=pltpu.VMEM), pl.BlockSpec(memory_space=pltpu.SMEM)
    return pl.pallas_call(
        rest_kernel,
        out_shape=jax.ShapeDtypeStruct((ASSETS, COLS), F32),
        in_specs=[smem, vmem, vmem, vmem, vmem, vmem],
        out_specs=pl.BlockSpec(memory_space=pltpu.HBM),
        scratch_shapes=[pltpu.VMEM((5, ROWS, SPAN), BF16)] * 2
        + [pltpu.VMEM((8 - FIRST, ROWS, COLS), F32), pltpu.SemaphoreType.DMA((8,))],
        compiler_params=pltpu.CompilerParams(vmem_limit_bytes=20 << 20),
    )(windows, whole, own, done, listed_from, listed_until)


def on_device(returns, windows, listed_from, listed_until):
    return completed(windows, *gathered(returns, windows, listed_from[None], listed_until[None]))[None]


def solution(mesh):
    placed = (P("tm", "asset"), P("tm"), P(), P())
    return jax.shard_map(
        on_device, mesh=mesh, in_specs=placed, out_specs=P("tm", None, "asset"), check_vma=False
    )
```

```python
import functools

import jax
import jax.numpy as jnp
from jax import lax
from jax.experimental import pallas as pl
from jax.experimental.pallas import tpu as pltpu
from jax.sharding import PartitionSpec as P

MESH = pl.DeviceIdType.MESH
F32, BF16 = jnp.float32, jnp.bfloat16
NZ, NX, NY = 8, 4, 4
GROUP, HALF, SPAN = 16, 8, 256
COLS, ASSETS = 512, 2048

Z_SEM = 0
YS_SEM = Z_SEM + 4
YSR_SEM = YS_SEM + 12
XA_SEM = YSR_SEM + 6
XAR_SEM = XA_SEM + 4
XB_SEM = XAR_SEM + 2
XBR_SEM = XB_SEM + 16
YA_SEM = XBR_SEM + 8
D_SEM = YA_SEM + 18
E_SEM = D_SEM + 4
N_SEM = E_SEM + 4


def gather_kernel(
    returns_ref,
    windows_ref,
    from_hbm,
    until_hbm,
    all_ref,
    own_ref,
    out_ref,
    from_ref,
    until_ref,
    back2,
    extra,
    wide_ref,
    ss,
    rs,
    local_sem,
):
    tm, y = lax.axis_index("tm"), lax.axis_index("asset")
    z, x, c = tm // 8, (tm // 2) % 4, tm % 2

    def dev(dz=0, dx=0, dy=0, dc=0):
        return (
            ((z + dz) % NZ) * 8 + ((x + dx) % NX) * 2 + (c + dc) % 2,
            (y + dy) % NY,
        )

    partner = dev(dc=1)

    def copy(src, dst, i, to):
        return pltpu.make_async_remote_copy(
            src_ref=src, dst_ref=dst, send_sem=ss.at[i], recv_sem=rs.at[i], device_id=to, device_id_type=MESH
        )

    def received(dst, i):
        copy(dst, dst, i, partner).wait_recv()

    def send(src, dst, i, to):
        copy(src, dst, i, to).start()

    def origin_block(h, at, k):
        return all_ref.at[at, c, h, x, k] if k < 2 else back2.at[h, at]

    loads = [
        pltpu.make_async_copy(returns_ref.at[pl.ds(h * HALF, HALF)], origin_block(h, y, 0), local_sem.at[h])
        for h in (0, 1)
    ]
    lists = [
        pltpu.make_async_copy(from_hbm, from_ref, local_sem.at[2]),
        pltpu.make_async_copy(until_hbm, until_ref, local_sem.at[3]),
    ]
    for load in loads + lists:
        load.start()
    barrier = pltpu.get_barrier_semaphore()

    def greet(peer):
        pl.semaphore_signal(barrier, inc=1, device_id=peer, device_id_type=MESH)

    flat = [dev(dx=1), dev(dx=-1), dev(dx=2), dev(dy=1), dev(dy=-1), dev(dy=2), partner]
    for k in (1, 2):
        pl.when(z >= k)(functools.partial(greet, dev(dz=-k)))
    for peer in flat:
        greet(peer)
    pl.semaphore_wait(barrier, len(flat) + jnp.minimum(NZ - 1 - z, 2))
    for load in loads + lists:
        load.wait()

    step = (1, -1)

    def ring_x(dx):
        return (x + dx) % NX

    def z_send(h, k):
        @pl.when(z + k < NZ)
        def _():
            send(origin_block(h, y, 0), origin_block(h, y, k), Z_SEM + h * 2 + k - 1, dev(dz=k))

    def z_wait(k):
        @pl.when(z >= k)
        def _():
            for h in (0, 1):
                received(origin_block(h, y, k), Z_SEM + h * 2 + k - 1)

    def y_sem(h, j, k):
        return YSR_SEM + h * 3 + k if j == 2 else YS_SEM + h * 6 + k * 2 + (0 if j == 3 else 1)

    def needed(h, k):
        return (z >= k) & (c == 1) if (h, k) == (0, 2) else z >= k

    def when_needed(h, k, go):
        go() if k == 0 else pl.when(needed(h, k))(go)

    def ys_send(js, k):
        for h in (1, 0):
            for j in js:
                block = origin_block(h, y, k)
                when_needed(h, k, functools.partial(send, block, block, y_sem(h, (NY - j) % NY, k), dev(dy=j)))

    def ys_wait(js, k):
        for j in js:
            at = (y + j) % NY
            for h in (1, 0):
                block = origin_block(h, at, k)
                when_needed(h, k, functools.partial(received, block, y_sem(h, j, k)))
                if k == 0:
                    above = functools.partial(send, block, origin_block(h, at, 1), y_sem(h, j, 1), dev(dz=1))
                    pl.when(z + 1 < NZ)(above)

    def x_sem(h, j, d, slot):
        near, far = (XA_SEM, XAR_SEM) if h == 0 else (XB_SEM + j * 4, XBR_SEM + j * 2)
        return far + slot if d == 2 else near + d * 2 + slot

    def with_slot(k, up, go):
        if k == 1:
            go(up.astype(jnp.int32))
        elif k == 0:
            pl.when(up)(functools.partial(go, 0))
        else:
            pl.when(jnp.logical_not(up))(functools.partial(go, 1))

    def x_send(h, j, k):
        at = (y + j) % NY
        for d, dx in ((2, 2), (0, 1), (1, -1)):

            def go(slot, d=d, dx=dx):
                send(origin_block(h, at, k), all_ref.at[at, c, h, x, slot], x_sem(h, j, d, slot), dev(dx=dx))

            with_slot(k, ring_x(dx) > x, go)

    def x_wait(h, j, k, far, then=None):
        at = (y + j) % NY
        for d, dx in ((2, 2),) if far else ((0, 1), (1, -1)):

            def go(slot, d=d, dx=dx):
                received(all_ref.at[at, c, h, ring_x(-dx), slot], x_sem(h, j, d, slot))
                if then is not None:
                    then(dx % NX, slot)

            with_slot(k, ring_x(-dx) < x, go)

    def ya_send(dist, slot, to=(1, 3)):
        view = all_ref.at[y, c, 0, ring_x(-dist), slot]
        for dy in to:
            send(view, view, YA_SEM + (dist - 1) * 6 + (dy - 1) * 2 + slot, dev(dy=dy))

    def ya_wait(j):
        for dist in (1, 3, 2):
            for slot in (0, 1):
                view = all_ref.at[(y + j) % NY, c, 0, ring_x(-dist), slot]
                received(view, YA_SEM + (dist - 1) * 6 + (3 - j) * 2 + slot)

    def x_all(h, j, ks=(0, 1, 2)):
        for k in ks:
            for far in (False, True):
                x_wait(h, j, k, far)

    def to_partner(j):
        at = (y + j) % NY
        send(all_ref.at[at, c], all_ref.at[at, c], D_SEM + j, partner)

        @pl.when(c == 1)
        def _():
            send(back2.at[:, at], extra.at[:, at], E_SEM + j, partner)

    def from_partner(j):
        at = (y + j) % NY
        received(all_ref.at[at, 1 - c], D_SEM + j)

        @pl.when(c == 0)
        def _():
            received(extra.at[:, at], E_SEM + j)
            all_ref[at, 1, :, x, 0] = extra[:, at]

    spans = spans_of(windows_ref, from_ref, until_ref, tm)
    own_spans = spans(pl.multiple_of(y * COLS, COLS), COLS)

    def some_rows(i):
        at, row = place_of(i, y)
        raw = all_ref[at].reshape(SPAN, COLS)[:, (i % 2) * ROWS : (i % 2 + 1) * ROWS]
        rows = prepare(raw, spans(row, ROWS), tm, wide_ref)
        correlate(wide_ref, rows, own_ref, own_spans, out_ref.at[pl.ds(i * ROWS, ROWS)])

    for k in (2, 1):
        for h in (1, 0):
            z_send(h, k)
    ys_send((2, 1, 3), 0)
    x_send(0, 0, 0)
    x_send(1, 0, 0)
    z_wait(1)
    x_send(0, 0, 1)
    x_send(1, 0, 1)
    z_wait(2)
    ys_send((2, 1, 3), 2)
    x_send(0, 0, 2)
    x_send(1, 0, 2)
    ys_wait((1, 3), 0)
    x_send(1, 1, 0)
    x_send(1, 3, 0)
    ys_wait((2,), 0)
    x_send(1, 2, 0)
    for k in (0, 1):
        x_wait(0, 0, k, False, ya_send)
        x_wait(0, 0, k, True, ya_send)
    ys_wait((1, 3), 1)
    x_send(1, 1, 1)
    x_send(1, 3, 1)
    ys_wait((1, 3), 2)
    x_send(1, 1, 2)
    x_send(1, 3, 2)
    ys_wait((2,), 2)
    x_send(1, 2, 2)
    x_wait(0, 0, 2, False, ya_send)
    x_wait(0, 0, 2, True, ya_send)
    for dist in (1, 3, 2):
        for slot in (0, 1):
            ya_send(dist, slot, (2,))
    ys_wait((2,), 1)
    x_send(1, 2, 1)
    x_all(1, 0)
    to_partner(0)

    from_partner(0)
    prepare_own(all_ref[y].reshape(SPAN, COLS), own_spans, tm, own_ref)
    some_rows(0)
    some_rows(1)
    x_all(1, 1)
    ya_wait(1)
    to_partner(1)
    x_all(1, 3)
    ya_wait(3)
    to_partner(3)
    x_all(1, 2)
    ya_wait(2)
    to_partner(2)
    from_partner(1)
    some_rows(2)
    some_rows(3)
    from_partner(3)
    some_rows(4)
    some_rows(5)
    from_partner(2)
    block, many = back2.at[0, 0], all_ref.at[0, 0]
    for i in range(E_SEM):
        view = many if i >= D_SEM else block
        done = copy(view, view, i, partner).wait_send
        if i < YS_SEM:
            pl.when(z + 1 + i % 2 < NZ)(done)
        elif i < XA_SEM:
            h, k = divmod(i - YSR_SEM, 3) if i >= YSR_SEM else divmod((i - YS_SEM) // 2, 3)
            pl.when(z + 1 < NZ)(done) if k == 1 else when_needed(h, k, done)
        else:
            done()

    @pl.when(c == 1)
    def _():
        for j in range(4):
            copy(back2.at[:, 0], extra.at[:, 0], E_SEM + j, partner).wait_send()


ROWS = 256
TILE = 256
ORDER = (0, 1, 3, 2)
FIRST = 6


def place_of(i, y):
    at = (y + ORDER[i // 2]) % NY
    return at, pl.multiple_of(at * COLS + (i % 2) * ROWS, ROWS)


def day_of(row, tm):
    core, half, at, slot, day = row // 128, (row // 64) % 2, (row // 16) % 4, (row // 8) % 2, row % 8
    place = at * 2 + core
    later = (at > (tm // 2) % 4).astype(jnp.int32)
    back = jnp.where((place == tm % 8 + 1) & (core == 1), 2 - slot, slot + later)
    return ((tm // 8 - back) * 8 + place) * GROUP + half * HALF + day


def split(value):
    high = value.astype(BF16)
    return high, (value - high.astype(F32)).astype(BF16)


def dot(left, right):
    return jnp.dot(left, right, preferred_element_type=F32)


def spans_of(windows_ref, from_ref, until_ref, tm):
    end = (tm + 1) * GROUP
    begin = jnp.maximum(end - windows_ref[0], 0)

    def spans(at, width):
        first = jnp.maximum(from_ref[:, pl.ds(at, width)], begin).astype(F32)
        last = jnp.minimum(until_ref[:, pl.ds(at, width)], end).astype(F32)
        return first, last

    return spans


def terms(day, first, last, raw, out_ref):
    live = (day >= first) & (day < last)
    value = jnp.where(live, raw, 0.0)
    out_ref[0] = live.astype(F32).astype(BF16)
    out_ref[1], out_ref[2] = split(value)
    out_ref[3], out_ref[4] = split(value * value)


def prepare_own(raw, spans, tm, own_ref):
    day = day_of(lax.broadcasted_iota(jnp.int32, (SPAN, 128), 0), tm).astype(F32)
    for n in range(0, COLS, 128):
        at = slice(n, n + 128)
        terms(day, spans[0][:, at], spans[1][:, at], raw[:, at], own_ref.at[:, :, pl.ds(n, 128)])


def prepare(raw, spans, tm, wide_ref):
    day = day_of(lax.broadcasted_iota(jnp.int32, (1, SPAN), 1), tm).astype(F32)
    first, last = (jnp.broadcast_to(span, (128, ROWS)).T for span in spans)
    for n in range(0, SPAN, 128):
        terms(day[:, n : n + 128], first, last, raw[n : n + 128].T, wide_ref.at[:, :, pl.ds(n, 128)])
    return first, last


def correlate(wide, rows, own_ref, own_spans, out_ref):
    first, last = rows
    live, high, low, sq_high, sq_low = (wide[i] for i in range(5))
    for n in range(0, COLS, TILE):
        at = slice(n, n + TILE)
        live_o, high_o, low_o, sq_high_o, sq_low_o = (own_ref[i, :, at] for i in range(5))
        cross = dot(high, high_o) + dot(low, high_o) + dot(high, low_o)
        sum_l = dot(high, live_o) + dot(low, live_o)
        square_l = dot(sq_high, live_o) + dot(sq_low, live_o)
        sum_r = dot(live, high_o) + dot(live, low_o)
        square_r = dot(live, sq_high_o) + dot(live, sq_low_o)
        pairs = jnp.concatenate(
            [
                jnp.minimum(last, own_spans[1][:, m : m + 128]) - jnp.maximum(first, own_spans[0][:, m : m + 128])
                for m in range(n, n + TILE, 128)
            ],
            axis=1,
        )
        pairs = jnp.maximum(pairs, 1.0)
        covariance = pairs * cross - sum_l * sum_r
        var_l = jnp.maximum(pairs * square_l - sum_l * sum_l, pairs)
        var_r = jnp.maximum(pairs * square_r - sum_r * sum_r, pairs)
        out_ref[:, at] = covariance * lax.rsqrt(var_l * var_r)


def gathered(returns, windows, listed_from, listed_until):
    vmem, smem, hbm = (pl.BlockSpec(memory_space=space) for space in (pltpu.VMEM, pltpu.SMEM, pltpu.HBM))
    returns, listed_from, listed_until = (
        pltpu.with_memory_space_constraint(array, pltpu.HBM) for array in (returns, listed_from, listed_until)
    )
    return pl.pallas_call(
        gather_kernel,
        out_shape=[
            jax.ShapeDtypeStruct((NY, 2, 2, NX, 2, HALF, COLS), F32),
            jax.ShapeDtypeStruct((5, SPAN, COLS), BF16),
            jax.ShapeDtypeStruct((FIRST * ROWS, COLS), F32),
            jax.ShapeDtypeStruct((1, ASSETS), jnp.int32),
            jax.ShapeDtypeStruct((1, ASSETS), jnp.int32),
        ],
        in_specs=[hbm, smem, hbm, hbm],
        out_specs=[vmem] * 5,
        scratch_shapes=[
            pltpu.VMEM((2, NY, HALF, COLS), F32),
            pltpu.VMEM((2, NY, HALF, COLS), F32),
            pltpu.VMEM((5, ROWS, SPAN), BF16),
            pltpu.SemaphoreType.DMA((N_SEM,)),
            pltpu.SemaphoreType.DMA((N_SEM,)),
            pltpu.SemaphoreType.DMA((4,)),
        ],
        compiler_params=pltpu.CompilerParams(collective_id=0, has_side_effects=True, vmem_limit_bytes=16 << 20),
    )(returns, windows, listed_from, listed_until)


def rest_kernel(windows_ref, all_ref, own_ref, done_ref, from_ref, until_ref, out_ref, wide_a, wide_b, result, sems):
    tm, y = lax.axis_index("tm"), lax.axis_index("asset")
    spans = spans_of(windows_ref, from_ref, until_ref, tm)
    own_spans = spans(pl.multiple_of(y * COLS, COLS), COLS)
    copies = []

    def store(src, i):
        copies.append(pltpu.make_async_copy(src, out_ref.at[pl.ds(place_of(i, y)[1], ROWS)], sems.at[i]))
        copies[-1].start()

    for i in range(FIRST):
        store(done_ref.at[pl.ds(i * ROWS, ROWS)], i)
    wides = wide_a, wide_b

    def ready(i):
        at, row = place_of(i, y)
        raw = all_ref[at].reshape(SPAN, COLS)[:, (i % 2) * ROWS : (i % 2 + 1) * ROWS]
        return prepare(raw, spans(row, ROWS), tm, wides[i % 2])

    rows = ready(FIRST)
    for i in range(FIRST, 8):
        now = rows
        if i < 7:
            rows = ready(i + 1)
        correlate(wides[i % 2], now, own_ref, own_spans, result.at[i - FIRST])
        store(result.at[i - FIRST], i)
    for copy in copies:
        copy.wait()


def completed(windows, whole, own, done, listed_from, listed_until):
    vmem, smem = pl.BlockSpec(memory_space=pltpu.VMEM), pl.BlockSpec(memory_space=pltpu.SMEM)
    return pl.pallas_call(
        rest_kernel,
        out_shape=jax.ShapeDtypeStruct((ASSETS, COLS), F32),
        in_specs=[smem, vmem, vmem, vmem, vmem, vmem],
        out_specs=pl.BlockSpec(memory_space=pltpu.HBM),
        scratch_shapes=[pltpu.VMEM((5, ROWS, SPAN), BF16)] * 2
        + [pltpu.VMEM((8 - FIRST, ROWS, COLS), F32), pltpu.SemaphoreType.DMA((8,))],
        compiler_params=pltpu.CompilerParams(vmem_limit_bytes=20 << 20),
    )(windows, whole, own, done, listed_from, listed_until)


def on_device(returns, windows, listed_from, listed_until):
    return completed(windows, *gathered(returns, windows, listed_from[None], listed_until[None]))[None]


def solution(mesh):
    placed = (P("tm", "asset"), P("tm"), P(), P())
    return jax.shard_map(
        on_device, mesh=mesh, in_specs=placed, out_specs=P("tm", None, "asset"), check_vma=False
    )
```

```python
import functools

import jax
import jax.numpy as jnp
from jax import lax
from jax.experimental import pallas as pl
from jax.experimental.pallas import tpu as pltpu
from jax.sharding import PartitionSpec as P

MESH = pl.DeviceIdType.MESH
F32, BF16 = jnp.float32, jnp.bfloat16
NZ, NX, NY = 8, 4, 4
GROUP, HALF, SPAN = 16, 8, 256
COLS, ASSETS = 512, 2048

Z_SEM = 0
YS_SEM = Z_SEM + 4
YSR_SEM = YS_SEM + 12
XA_SEM = YSR_SEM + 6
XAR_SEM = XA_SEM + 4
XB_SEM = XAR_SEM + 2
XBR_SEM = XB_SEM + 16
YA_SEM = XBR_SEM + 8
D_SEM = YA_SEM + 18
E_SEM = D_SEM + 4
N_SEM = E_SEM + 4


def gather_kernel(
    returns_ref,
    windows_ref,
    from_hbm,
    until_hbm,
    all_ref,
    own_ref,
    out_ref,
    from_ref,
    until_ref,
    back2,
    extra,
    wide_ref,
    ss,
    rs,
    local_sem,
):
    tm, y = lax.axis_index("tm"), lax.axis_index("asset")
    z, x, c = tm // 8, (tm // 2) % 4, tm % 2

    def dev(dz=0, dx=0, dy=0, dc=0):
        return (
            ((z + dz) % NZ) * 8 + ((x + dx) % NX) * 2 + (c + dc) % 2,
            (y + dy) % NY,
        )

    partner = dev(dc=1)

    def copy(src, dst, i, to):
        return pltpu.make_async_remote_copy(
            src_ref=src, dst_ref=dst, send_sem=ss.at[i], recv_sem=rs.at[i], device_id=to, device_id_type=MESH
        )

    def received(dst, i):
        copy(dst, dst, i, partner).wait_recv()

    def send(src, dst, i, to):
        copy(src, dst, i, to).start()

    def origin_block(h, at, k):
        return all_ref.at[at, c, h, x, k] if k < 2 else back2.at[h, at]

    loads = [
        pltpu.make_async_copy(returns_ref.at[pl.ds(h * HALF, HALF)], origin_block(h, y, 0), local_sem.at[h])
        for h in (0, 1)
    ]
    lists = [
        pltpu.make_async_copy(from_hbm, from_ref, local_sem.at[2]),
        pltpu.make_async_copy(until_hbm, until_ref, local_sem.at[3]),
    ]
    for load in loads + lists:
        load.start()
    barrier = pltpu.get_barrier_semaphore()

    def greet(peer):
        pl.semaphore_signal(barrier, inc=1, device_id=peer, device_id_type=MESH)

    flat = [dev(dx=1), dev(dx=-1), dev(dx=2), dev(dy=1), dev(dy=-1), dev(dy=2), partner]
    for k in (1, 2):
        pl.when(z >= k)(functools.partial(greet, dev(dz=-k)))
    for peer in flat:
        greet(peer)
    pl.semaphore_wait(barrier, len(flat) + jnp.minimum(NZ - 1 - z, 2))
    for load in loads + lists:
        load.wait()

    step = (1, -1)

    def ring_x(dx):
        return (x + dx) % NX

    def z_send(h, k):
        @pl.when(z + k < NZ)
        def _():
            send(origin_block(h, y, 0), origin_block(h, y, k), Z_SEM + h * 2 + k - 1, dev(dz=k))

    def z_wait(k):
        @pl.when(z >= k)
        def _():
            for h in (0, 1):
                received(origin_block(h, y, k), Z_SEM + h * 2 + k - 1)

    def y_sem(h, j, k):
        return YSR_SEM + h * 3 + k if j == 2 else YS_SEM + h * 6 + k * 2 + (0 if j == 3 else 1)

    def needed(h, k):
        return (z >= k) & (c == 1) if (h, k) == (0, 2) else z >= k

    def when_needed(h, k, go):
        go() if k == 0 else pl.when(needed(h, k))(go)

    def ys_send(js, k):
        for h in (1, 0):
            for j in js:
                block = origin_block(h, y, k)
                when_needed(h, k, functools.partial(send, block, block, y_sem(h, (NY - j) % NY, k), dev(dy=j)))

    def ys_wait(js, k):
        for j in js:
            at = (y + j) % NY
            for h in (1, 0):
                block = origin_block(h, at, k)
                when_needed(h, k, functools.partial(received, block, y_sem(h, j, k)))
                if k == 0:
                    above = functools.partial(send, block, origin_block(h, at, 1), y_sem(h, j, 1), dev(dz=1))
                    pl.when(z + 1 < NZ)(above)

    def x_sem(h, j, d, slot):
        near, far = (XA_SEM, XAR_SEM) if h == 0 else (XB_SEM + j * 4, XBR_SEM + j * 2)
        return far + slot if d == 2 else near + d * 2 + slot

    def with_slot(k, up, go):
        if k == 1:
            go(up.astype(jnp.int32))
        elif k == 0:
            pl.when(up)(functools.partial(go, 0))
        else:
            pl.when(jnp.logical_not(up))(functools.partial(go, 1))

    def x_send(h, j, k):
        at = (y + j) % NY
        for d, dx in ((2, 2), (0, 1), (1, -1)):

            def go(slot, d=d, dx=dx):
                send(origin_block(h, at, k), all_ref.at[at, c, h, x, slot], x_sem(h, j, d, slot), dev(dx=dx))

            with_slot(k, ring_x(dx) > x, go)

    def x_wait(h, j, k, far, then=None):
        at = (y + j) % NY
        for d, dx in ((2, 2),) if far else ((0, 1), (1, -1)):

            def go(slot, d=d, dx=dx):
                received(all_ref.at[at, c, h, ring_x(-dx), slot], x_sem(h, j, d, slot))
                if then is not None:
                    then(dx % NX, slot)

            with_slot(k, ring_x(-dx) < x, go)

    def ya_send(dist, slot, to=(1, 3)):
        view = all_ref.at[y, c, 0, ring_x(-dist), slot]
        for dy in to:
            send(view, view, YA_SEM + (dist - 1) * 6 + (dy - 1) * 2 + slot, dev(dy=dy))

    def ya_wait(j):
        for dist in (1, 3, 2):
            for slot in (0, 1):
                view = all_ref.at[(y + j) % NY, c, 0, ring_x(-dist), slot]
                received(view, YA_SEM + (dist - 1) * 6 + (3 - j) * 2 + slot)

    def x_all(h, j, ks=(0, 1, 2)):
        for k in ks:
            for far in (False, True):
                x_wait(h, j, k, far)

    def to_partner(j):
        at = (y + j) % NY
        send(all_ref.at[at, c], all_ref.at[at, c], D_SEM + j, partner)

        @pl.when(c == 1)
        def _():
            send(back2.at[:, at], extra.at[:, at], E_SEM + j, partner)

    def from_partner(j):
        at = (y + j) % NY
        received(all_ref.at[at, 1 - c], D_SEM + j)

        @pl.when(c == 0)
        def _():
            received(extra.at[:, at], E_SEM + j)
            all_ref[at, 1, :, x, 0] = extra[:, at]

    spans = spans_of(windows_ref, from_ref, until_ref, tm)
    own_spans = spans(pl.multiple_of(y * COLS, COLS), COLS)

    def some_rows(i):
        at, row = place_of(i, y)
        raw = all_ref[at].reshape(SPAN, COLS)[:, (i % 2) * ROWS : (i % 2 + 1) * ROWS]
        rows = prepare(raw, spans(row, ROWS), tm, wide_ref)
        correlate(wide_ref, rows, own_ref, own_spans, out_ref.at[pl.ds(i * ROWS, ROWS)])

    for k in (2, 1):
        for h in (1, 0):
            z_send(h, k)
    ys_send((2, 1, 3), 0)
    x_send(0, 0, 0)
    x_send(1, 0, 0)
    z_wait(1)
    x_send(0, 0, 1)
    x_send(1, 0, 1)
    z_wait(2)
    ys_send((2, 1, 3), 2)
    x_send(0, 0, 2)
    x_send(1, 0, 2)
    ys_wait((1, 3), 0)
    x_send(1, 1, 0)
    x_send(1, 3, 0)
    ys_wait((2,), 0)
    x_send(1, 2, 0)
    for k in (0, 1):
        x_wait(0, 0, k, False, ya_send)
        x_wait(0, 0, k, True, ya_send)
    ys_wait((1, 3), 1)
    x_send(1, 1, 1)
    x_send(1, 3, 1)
    ys_wait((1, 3), 2)
    x_send(1, 1, 2)
    x_send(1, 3, 2)
    ys_wait((2,), 2)
    x_send(1, 2, 2)
    x_wait(0, 0, 2, False, ya_send)
    x_wait(0, 0, 2, True, ya_send)
    for dist in (1, 3, 2):
        for slot in (0, 1):
            ya_send(dist, slot, (2,))
    ys_wait((2,), 1)
    x_send(1, 2, 1)
    x_all(1, 0)
    to_partner(0)

    from_partner(0)
    prepare_own(all_ref[y].reshape(SPAN, COLS), own_spans, tm, own_ref)
    some_rows(0)
    some_rows(1)
    x_all(1, 1)
    ya_wait(1)
    to_partner(1)
    x_all(1, 3)
    ya_wait(3)
    to_partner(3)
    x_all(1, 2)
    ya_wait(2)
    to_partner(2)
    from_partner(1)
    some_rows(2)
    some_rows(3)
    from_partner(3)
    some_rows(4)
    some_rows(5)
    from_partner(2)
    block, many = back2.at[0, 0], all_ref.at[0, 0]
    for i in range(E_SEM):
        view = many if i >= D_SEM else block
        done = copy(view, view, i, partner).wait_send
        if i < YS_SEM:
            pl.when(z + 1 + i % 2 < NZ)(done)
        elif i < XA_SEM:
            h, k = divmod(i - YSR_SEM, 3) if i >= YSR_SEM else divmod((i - YS_SEM) // 2, 3)
            pl.when(z + 1 < NZ)(done) if k == 1 else when_needed(h, k, done)
        else:
            done()

    @pl.when(c == 1)
    def _():
        for j in range(4):
            copy(back2.at[:, 0], extra.at[:, 0], E_SEM + j, partner).wait_send()


ROWS = 256
TILE = 256
ORDER = (0, 1, 3, 2)
FIRST = 6


def place_of(i, y):
    at = (y + ORDER[i // 2]) % NY
    return at, pl.multiple_of(at * COLS + (i % 2) * ROWS, ROWS)


def day_of(row, tm):
    core, half, at, slot, day = row // 128, (row // 64) % 2, (row // 16) % 4, (row // 8) % 2, row % 8
    place = at * 2 + core
    later = (at > (tm // 2) % 4).astype(jnp.int32)
    back = jnp.where((place == tm % 8 + 1) & (core == 1), 2 - slot, slot + later)
    return ((tm // 8 - back) * 8 + place) * GROUP + half * HALF + day


def split(value):
    high = value.astype(BF16)
    return high, (value - high.astype(F32)).astype(BF16)


def dot(left, right):
    return jnp.dot(left, right, preferred_element_type=F32)


def spans_of(windows_ref, from_ref, until_ref, tm):
    end = (tm + 1) * GROUP
    begin = jnp.maximum(end - windows_ref[0], 0)

    def spans(at, width):
        first = jnp.maximum(from_ref[:, pl.ds(at, width)], begin).astype(F32)
        last = jnp.minimum(until_ref[:, pl.ds(at, width)], end).astype(F32)
        return first, last

    return spans


def terms(day, first, last, raw, out_ref):
    live = (day >= first) & (day < last)
    value = jnp.where(live, raw, 0.0)
    out_ref[0] = live.astype(F32).astype(BF16)
    out_ref[1], out_ref[2] = split(value)
    out_ref[3], out_ref[4] = split(value * value)


def prepare_own(raw, spans, tm, own_ref):
    day = day_of(lax.broadcasted_iota(jnp.int32, (SPAN, 128), 0), tm).astype(F32)
    for n in range(0, COLS, 128):
        at = slice(n, n + 128)
        terms(day, spans[0][:, at], spans[1][:, at], raw[:, at], own_ref.at[:, :, pl.ds(n, 128)])


def prepare(raw, spans, tm, wide_ref):
    day = day_of(lax.broadcasted_iota(jnp.int32, (1, SPAN), 1), tm).astype(F32)
    first, last = (jnp.broadcast_to(span, (128, ROWS)).T for span in spans)
    for n in range(0, SPAN, 128):
        terms(day[:, n : n + 128], first, last, raw[n : n + 128].T, wide_ref.at[:, :, pl.ds(n, 128)])
    return first, last


def correlate(wide, rows, own_ref, own_spans, out_ref, after=None):
    first, last = rows
    live, high, low, sq_high, sq_low = (wide[i] for i in range(5))
    for n in range(0, COLS, TILE):
        at = slice(n, n + TILE)
        live_o, high_o, low_o, sq_high_o, sq_low_o = (own_ref[i, :, at] for i in range(5))
        cross = dot(high, high_o) + dot(low, high_o) + dot(high, low_o)
        sum_l = dot(high, live_o) + dot(low, live_o)
        square_l = dot(sq_high, live_o) + dot(sq_low, live_o)
        sum_r = dot(live, high_o) + dot(live, low_o)
        square_r = dot(live, sq_high_o) + dot(live, sq_low_o)
        pairs = jnp.concatenate(
            [
                jnp.minimum(last, own_spans[1][:, m : m + 128]) - jnp.maximum(first, own_spans[0][:, m : m + 128])
                for m in range(n, n + TILE, 128)
            ],
            axis=1,
        )
        pairs = jnp.maximum(pairs, 1.0)
        covariance = pairs * cross - sum_l * sum_r
        var_l = jnp.maximum(pairs * square_l - sum_l * sum_l, pairs)
        var_r = jnp.maximum(pairs * square_r - sum_r * sum_r, pairs)
        out_ref[:, at] = covariance * lax.rsqrt(var_l * var_r)
        if after is not None:
            after(n)


def gathered(returns, windows, listed_from, listed_until):
    vmem, smem, hbm = (pl.BlockSpec(memory_space=space) for space in (pltpu.VMEM, pltpu.SMEM, pltpu.HBM))
    returns, listed_from, listed_until = (
        pltpu.with_memory_space_constraint(array, pltpu.HBM) for array in (returns, listed_from, listed_until)
    )
    return pl.pallas_call(
        gather_kernel,
        out_shape=[
            jax.ShapeDtypeStruct((NY, 2, 2, NX, 2, HALF, COLS), F32),
            jax.ShapeDtypeStruct((5, SPAN, COLS), BF16),
            jax.ShapeDtypeStruct((FIRST * ROWS, COLS), F32),
            jax.ShapeDtypeStruct((1, ASSETS), jnp.int32),
            jax.ShapeDtypeStruct((1, ASSETS), jnp.int32),
        ],
        in_specs=[hbm, smem, hbm, hbm],
        out_specs=[vmem] * 5,
        scratch_shapes=[
            pltpu.VMEM((2, NY, HALF, COLS), F32),
            pltpu.VMEM((2, NY, HALF, COLS), F32),
            pltpu.VMEM((5, ROWS, SPAN), BF16),
            pltpu.SemaphoreType.DMA((N_SEM,)),
            pltpu.SemaphoreType.DMA((N_SEM,)),
            pltpu.SemaphoreType.DMA((4,)),
        ],
        compiler_params=pltpu.CompilerParams(collective_id=0, has_side_effects=True, vmem_limit_bytes=16 << 20),
    )(returns, windows, listed_from, listed_until)


def rest_kernel(windows_ref, all_ref, own_ref, done_ref, from_ref, until_ref, out_ref, wide_a, wide_b, result, sems):
    tm, y = lax.axis_index("tm"), lax.axis_index("asset")
    spans = spans_of(windows_ref, from_ref, until_ref, tm)
    own_spans = spans(pl.multiple_of(y * COLS, COLS), COLS)
    copies = []

    def store(src, i):
        copies.append(pltpu.make_async_copy(src, out_ref.at[pl.ds(place_of(i, y)[1], ROWS)], sems.at[i]))
        copies[-1].start()

    for i in range(FIRST):
        store(done_ref.at[pl.ds(i * ROWS, ROWS)], i)
    wides = wide_a, wide_b

    def ready(i):
        at, row = place_of(i, y)
        raw = all_ref[at].reshape(SPAN, COLS)[:, (i % 2) * ROWS : (i % 2 + 1) * ROWS]
        return prepare(raw, spans(row, ROWS), tm, wides[i % 2])

    rows = ready(FIRST)
    for i in range(FIRST, 8):
        now = rows
        if i < 7:
            rows = ready(i + 1)

        def tile_done(n, i=i):
            rows_of, cols = pl.ds(place_of(i, y)[1], ROWS), pl.ds(n, TILE)
            src = result.at[i - FIRST, :, cols]
            copies.append(pltpu.make_async_copy(src, out_ref.at[rows_of, cols], sems.at[i + n // TILE]))
            copies[-1].start()

        correlate(wides[i % 2], now, own_ref, own_spans, result.at[i - FIRST], tile_done if i == 7 else None)
        if i < 7:
            store(result.at[i - FIRST], i)
    for copy in copies:
        copy.wait()


def completed(windows, whole, own, done, listed_from, listed_until):
    vmem, smem = pl.BlockSpec(memory_space=pltpu.VMEM), pl.BlockSpec(memory_space=pltpu.SMEM)
    return pl.pallas_call(
        rest_kernel,
        out_shape=jax.ShapeDtypeStruct((ASSETS, COLS), F32),
        in_specs=[smem, vmem, vmem, vmem, vmem, vmem],
        out_specs=pl.BlockSpec(memory_space=pltpu.HBM),
        scratch_shapes=[pltpu.VMEM((5, ROWS, SPAN), BF16)] * 2
        + [pltpu.VMEM((8 - FIRST, ROWS, COLS), F32), pltpu.SemaphoreType.DMA((9,))],
        compiler_params=pltpu.CompilerParams(vmem_limit_bytes=20 << 20),
    )(windows, whole, own, done, listed_from, listed_until)


def on_device(returns, windows, listed_from, listed_until):
    return completed(windows, *gathered(returns, windows, listed_from[None], listed_until[None]))[None]


def solution(mesh):
    placed = (P("tm", "asset"), P("tm"), P(), P())
    return jax.shard_map(
        on_device, mesh=mesh, in_specs=placed, out_specs=P("tm", None, "asset"), check_vma=False
    )
```
